256 devices in a mesh: dp: 8 (over y_lo, x), ctx: 32 (over y_hi, z, core).
Axes of the slice: x: 4, y: 4 (y_hi: 2, y_lo: 2; y = y_hi * 2 + y_lo), z: 8, core: 2. Of those that a mesh axis runs over, the one named last changes fastest.
Arguments:
- query_rows: bfloat16 [32768, 2048], P(('dp', 'ctx')), may hold values from -64 to 64
- key_rows: bfloat16 [32768, 2048], P(('dp', 'ctx')), may hold values from -64 to 64
- value_rows: bfloat16 [32768, 2048], P(('dp', 'ctx')), may hold values from -6 to 6
- cotangent: bfloat16 [32768, 2048], P(('dp', 'ctx')), may hold values from -6 to 6
- query_gain: float32 [2048], replicated, may hold values from 0.5 to 5.5
- key_gain: float32 [2048], replicated, may hold values from 0.5 to 5.5
- positions: int32 [32768], P(('dp', 'ctx')), may hold values from 0 to 2047, as said below
- span_start: int32 [16, 2], P('dp'), may hold values from 0 to 1536, as said below
- span_length: int32 [16, 2], P('dp'), may hold values from 256 to 512
Outputs:
- output: bfloat16 [32768, 2048], P(('dp', 'ctx'))
- query_grad: bfloat16 [32768, 2048], P(('dp', 'ctx'))
- key_grad: bfloat16 [32768, 2048], P(('dp', 'ctx'))
- value_grad: bfloat16 [32768, 2048], P(('dp', 'ctx'))
- gain_grads: float32 [2, 2048], replicated
The draws below stay inside these ranges and needn't reach their ends.
Inputs may be any that keep to these rules, and one draw needn't show every extreme that they name: Within each sequence every position 0 to 2047 appears once; each block's rows are two runs of 64 consecutive positions, each run in increasing order. `span_start`: the first span of a sequence starts at 512 or earlier, the second at 1024 or later; spans don't intersect and end inside the sequence.
All inputs are finite; a program needn't handle non-finite values.
Results may differ from the reference program's by a relative error of at most 0.035.
The reference program's roundings to bfloat16 on the way count: a program that leaves them out, or rounds other values in their place, can miss the bound.
Values may be sent and summed in bfloat16 or wider, within the bound.
A program may use at most 128 MiB of HBM per device.

```python
import jax
import jax.numpy as jnp
from jax import lax

HEADS = 16
HEAD = 128
TOK_DEV = 128
SEQS_CTX = 2
NSPAN = 2
CYCLE = 16
LEN = 2048
SPAN = 512
PIECE = 64
NSEQ = 16
ROWS = 32768
N_DP = 8


def query_base(key):
    sample_draw = jax.random.normal(jax.random.fold_in(key, 101), (ROWS, HEADS * HEAD), jnp.float32)
    return jnp.clip(sample_draw, -64.0, 64.0)


def draw_query_rows(key, part):
    return query_base(key).astype(jnp.bfloat16)


def draw_key_rows(key, part):
    fresh_keys = jax.random.normal(jax.random.fold_in(key, 201), (ROWS, HEADS * HEAD), jnp.float32)
    return jnp.clip(fresh_keys, -64.0, 64.0).astype(jnp.bfloat16)


def gain_draw(key, salt_id):
    channel = jax.random.uniform(jax.random.fold_in(key, salt_id), (HEADS, HEAD), jnp.float32, 0.6, 1.6)
    return channel.reshape(HEADS * HEAD).astype(jnp.float32)


def draw_query_gain(key, part):
    return gain_draw(key, 302)


def draw_key_gain(key, part):
    return gain_draw(key, 303)


def draw_positions(key, part):
    seq_keys = jax.random.split(jax.random.fold_in(key, 501), NSEQ)
    orders = jax.vmap(lambda single: jax.random.permutation(single, 2 * CYCLE))(seq_keys)
    orders = orders.reshape(N_DP, SEQS_CTX, CYCLE, 2)
    orders = jnp.transpose(orders, (0, 2, 1, 3))
    places = orders[..., None] * PIECE + jnp.arange(PIECE, dtype=jnp.int32)
    return places.reshape(ROWS).astype(jnp.int32)


def draw_span_start(key, part):
    first_start = jax.random.randint(jax.random.fold_in(key, 401), (NSEQ,), 0, LEN // 2 - SPAN + 1)
    second = jax.random.randint(jax.random.fold_in(key, 402), (NSEQ,), LEN // 2, LEN - SPAN + 1)
    return jnp.stack([first_start, second], axis=1).astype(jnp.int32)


def set_ends(result, rng, smallest, largest):
    extent = result.shape
    place = [jax.random.randint(jax.random.fold_in(rng, axis), (), 0, extent[axis]) for axis in range(len(extent))]
    result = result.at[tuple(place)].set(smallest)
    longest = extent.index(max(extent))
    place[longest] = (place[longest] + 1) % extent[longest]
    return result.at[tuple(place)].set(largest)


def shard_levels(key, extent, pieces, least, largest):
    factor_of, own = 1.0, jax.random.fold_in(key, 6)
    for position, shards_of in pieces:
        draws = jnp.exp(jax.random.uniform(jax.random.fold_in(own, position), (shards_of,), jnp.float32, least / len(pieces), largest / len(pieces)))
        factor_of = factor_of * jnp.repeat(draws, extent[position] // shards_of).reshape([-1 if axis == position else 1 for axis in range(len(extent))])
    return factor_of


def scatter_about(key, extent, spread, most, pieces=(), kind=jnp.bfloat16):
    array = jax.random.normal(key, extent, jnp.float32) * spread
    if len(pieces) > 0:
        array = shard_levels(key, extent, pieces, -0.22, 0.18) * array
    return jnp.clip(array, min=-most, max=most).astype(kind)


def setup_inputs(seed: int = 0) -> dict:
    splits = jax.random.split(jax.random.key(seed), 10)
    return {
        "query_rows": draw_query_rows(jax.random.fold_in(splits[9], 71), 0),
        "key_rows": draw_key_rows(jax.random.fold_in(splits[9], 71), 0),
        "value_rows": scatter_about(splits[2], (ROWS, HEADS * HEAD), 1.0, 6.0, ((0, 256),)),
        "cotangent": scatter_about(splits[3], (ROWS, HEADS * HEAD), 1.0, 6.0, ((0, 256),)),
        "query_gain": draw_query_gain(jax.random.fold_in(splits[9], 71), 0),
        "key_gain": draw_key_gain(jax.random.fold_in(splits[9], 71), 0),
        "positions": draw_positions(jax.random.fold_in(splits[9], 71), 0),
        "span_start": draw_span_start(jax.random.fold_in(splits[9], 71), 0),
        "span_length": set_ends(jax.random.randint(splits[8], (NSEQ, NSPAN), SPAN // 2, SPAN + 1), jax.random.fold_in(splits[8], 1), SPAN // 2, SPAN).astype(jnp.int32),
    }


epsilon = 1e-05
masked_score = -1e+30

def normalize(raw_rows, gain_row):
    values = raw_rows.astype(jnp.float32).reshape(raw_rows.shape[0], HEADS, HEAD)
    inverse = lax.rsqrt(lax.optimization_barrier(jnp.mean(values * values, axis=-1, keepdims=True)) + epsilon)
    unit_rows = values * inverse
    return (unit_rows, inverse, (unit_rows * gain_row.reshape(HEADS, HEAD)).astype(jnp.bfloat16))

def norm_backward(grad_normed, unit_rows, inverse, gain_row):
    grad_unit = grad_normed * gain_row.reshape(HEADS, HEAD)
    projected = lax.optimization_barrier(jnp.mean(grad_unit * unit_rows, axis=-1, keepdims=True))
    grad_raw = inverse * (grad_unit - unit_rows * projected)
    gain_part = lax.optimization_barrier(jnp.sum(grad_normed * unit_rows, axis=0)).reshape(HEADS * HEAD)
    return (grad_raw.reshape(grad_raw.shape[0], HEADS * HEAD).astype(jnp.bfloat16), gain_part)

def span_labels(places, starts, lengths):
    inside = (places[:, None] >= starts[None, :]) & (places[:, None] < starts[None, :] + lengths[None, :])
    span_ids = jnp.arange(1, starts.shape[0] + 1, dtype=jnp.int32)
    return lax.optimization_barrier(jnp.sum(jnp.where(inside, span_ids[None, :], 0), axis=1)).astype(jnp.int32)

def visible(query_places, query_labels, key_places, key_labels):
    causal = key_places[None, :] <= query_places[:, None]
    same_span = (query_labels[:, None] == key_labels[None, :]) & (query_labels[:, None] > 0)
    return causal | same_span

def to_sequences(tensor):
    trailing = tensor.shape[1:]
    shaped = tensor.reshape((N_DP, CYCLE, SEQS_CTX, TOK_DEV) + trailing)
    return jnp.swapaxes(shaped, 1, 2).reshape((NSEQ, LEN) + trailing)

def from_sequences(tensor):
    trailing = tensor.shape[2:]
    shaped = tensor.reshape((N_DP, SEQS_CTX, CYCLE, TOK_DEV) + trailing)
    return jnp.swapaxes(shaped, 1, 2).reshape((ROWS,) + trailing)

def rounded(tensor):
    return lax.optimization_barrier(tensor.astype(jnp.bfloat16)).astype(jnp.float32)

def one_sequence(packed):
    query_normed, key_normed, value_block, out_grads, places, starts, lengths = packed
    score_scale = HEAD ** (-0.5)
    labels = span_labels(places, starts, lengths)
    allowed = visible(places, labels, places, labels)

    def one_head(head_pack):
        query_float, key_float, value_float, grad_float = head_pack
        scores = jnp.einsum('qd,kd->qk', query_float, key_float) * score_scale
        scores = jnp.where(allowed, scores, masked_score)
        row_max = lax.optimization_barrier(jnp.max(scores, axis=-1, keepdims=True))
        log_total = row_max + jnp.log(lax.optimization_barrier(jnp.sum(jnp.exp(scores - row_max), axis=-1, keepdims=True)))
        attn_probs = jnp.exp(scores - log_total)
        weights = rounded(attn_probs)
        output = jnp.einsum('qk,kd->qd', weights, value_float)
        row_delta = lax.optimization_barrier(jnp.sum(rounded(output) * grad_float, axis=-1, keepdims=True))
        grad_values = jnp.einsum('qk,qd->kd', weights, grad_float).astype(jnp.bfloat16)
        prob_grads = jnp.einsum('qd,kd->qk', grad_float, value_float)
        score_grads = rounded(attn_probs * (prob_grads - row_delta))
        grad_query = jnp.einsum('qk,kd->qd', score_grads, key_float) * score_scale
        grad_keys = jnp.einsum('qk,qd->kd', score_grads, query_float) * score_scale
        return (output.astype(jnp.bfloat16), grad_values, grad_query, grad_keys)
    head_major = tuple((jnp.transpose(tensor.astype(jnp.float32), (1, 0, 2)) for tensor in (query_normed, key_normed, value_block, out_grads)))
    results = lax.map(one_head, head_major)
    return tuple((jnp.transpose(tensor, (1, 0, 2)) for tensor in results))

def reference(query_rows, key_rows, value_rows, cotangent, query_gain, key_gain, positions, span_start, span_length):
    query_unit, query_inverse, query_normed = normalize(query_rows, query_gain)
    key_unit, key_inverse, key_normed = normalize(key_rows, key_gain)
    packed = (to_sequences(query_normed), to_sequences(key_normed), to_sequences(value_rows.reshape(ROWS, HEADS, HEAD)), to_sequences(cotangent.reshape(ROWS, HEADS, HEAD)), to_sequences(positions), span_start, span_length)
    output, grad_values, grad_query, grad_keys = lax.map(one_sequence, packed)
    output = from_sequences(output).reshape(ROWS, HEADS * HEAD)
    value_grad = from_sequences(grad_values).reshape(ROWS, HEADS * HEAD)
    query_grad, query_part = norm_backward(from_sequences(grad_query), query_unit, query_inverse, query_gain)
    key_grad, key_part = norm_backward(from_sequences(grad_keys), key_unit, key_inverse, key_gain)
    gain_grads = jnp.stack([query_part, key_part])
    return (output, query_grad, key_grad, value_grad, gain_grads)
```

```python
import functools

import jax
import jax.numpy as jnp
from jax import lax
from jax.experimental import pallas as pl
from jax.experimental.pallas import tpu as pltpu
from jax.sharding import Mesh
from jax.sharding import PartitionSpec as P

HEADS = 16
HEAD = 128
PEERS = ("ctx_0", "ctx_1")
DP_CTX = ("dp_0", "dp_1", "ctx_0", "ctx_1", "ctx_2")
DP = ("dp_0", "dp_1")
EPS = 1e-05
MASKED = -1e30
SCALE = HEAD**-0.5
LOG2E = 1.4426950408889634
F32 = jnp.float32
BF16 = jnp.bfloat16

TOK = 128
MEMBERS = 16
LEN = TOK * MEMBERS
PER = 2
QB = TOK * PER
STEPS = MEMBERS // PER
KC = 256
CHUNKS = LEN // KC


def unit_of(raw):
    values = raw.astype(F32)
    inverse = lax.rsqrt(jnp.mean(values * values, axis=-1, keepdims=True) + EPS)
    return values * inverse, inverse


def norm_back(grad, raw, gain):
    unit, inverse = unit_of(raw)
    u = grad * gain
    projected = jnp.mean(u * unit, axis=-1, keepdims=True)
    part = jnp.sum(grad * unit, axis=0, keepdims=True)
    return (inverse * (u - unit * projected)).astype(BF16), part


def dot(a, b):
    return jnp.dot(a, b, preferred_element_type=F32)


def fold8(x, op):
    return op(x.reshape(x.shape[0] // 8, 8, x.shape[1]), axis=0)


def place_masks(pos_ref, spans, kpos_ref, limit_ref):
    places = pos_ref[...]
    limit = places + 1.0
    for start, end in spans:
        limit = jnp.where((places >= start) & (places < end), end, limit)
    for b in range(STEPS):
        limit_ref[b] = jnp.concatenate(
            [limit[b * PER + i : b * PER + i + 1, :] for i in range(PER)], axis=1
        )
    for r in range(MEMBERS):
        row = jnp.broadcast_to(places[r : r + 1, :], (TOK, TOK))
        kpos_ref[r * TOK : (r + 1) * TOK, :] = row.T


def prepare_keys(k_ref, v_ref, kgain, kn_ref, knT_ref, vT_ref):
    for r in range(MEMBERS):
        rows = slice(r * TOK, (r + 1) * TOK)
        unit, _ = unit_of(k_ref[r])
        normed = unit * kgain
        kn_ref[rows, :] = normed.astype(BF16)
        knT_ref[:, rows] = normed.T.astype(BF16)
        vT_ref[:, rows] = v_ref[r].astype(F32).T.astype(BF16)


def query_step(
    b, q_ref, do_ref, v_ref, qgain, kn_ref, knT_ref, vT_ref, kpos_ref, limit_ref, s_ref, p_ref, dk_ref, dv_ref, gq_ref
):
    raw = q_ref[pl.ds(b * PER, PER)].reshape(QB, HEAD)
    unit, _ = unit_of(raw)
    normed = unit * qgain
    qn = normed.astype(BF16)
    qnT = normed.T.astype(BF16)
    limit = limit_ref[b]
    top = jnp.full((8, QB), MASKED, F32)
    for j in range(CHUNKS):
        rows = slice(j * KC, (j + 1) * KC)
        kp = kpos_ref[rows, :]
        kp = jnp.concatenate([kp] * (QB // 128), axis=1)
        s = jnp.where(kp < limit, dot(kn_ref[rows, :], qnT) * (SCALE * LOG2E), MASKED)
        s_ref[rows, :] = s
        top = jnp.maximum(top, fold8(s, jnp.max))
    top = jnp.max(top, axis=0, keepdims=True)
    total = jnp.zeros((8, QB), F32)
    oT = jnp.zeros((HEAD, QB), F32)
    for j in range(CHUNKS):
        rows = slice(j * KC, (j + 1) * KC)
        p = jnp.exp2(s_ref[rows, :] - top)
        total = total + fold8(p, jnp.sum)
        pb = p.astype(BF16)
        p_ref[rows, :] = pb
        oT = oT + dot(vT_ref[:, rows], pb)
    inv = 1.0 / jnp.sum(total, axis=0, keepdims=True)
    oT = (oT * inv).astype(BF16).astype(F32)
    out = oT.T.astype(BF16)
    gradT = do_ref[pl.ds(b * PER, PER)].reshape(QB, HEAD).astype(F32).T * inv
    gT = gradT.astype(BF16)
    gT32 = gT.astype(F32)
    g = gT32.T.astype(BF16)
    delta = jnp.sum(oT * gT32, axis=0, keepdims=True)
    dqT = jnp.zeros((HEAD, QB), F32)
    for j in range(CHUNKS):
        rows = slice(j * KC, (j + 1) * KC)
        per = KC // TOK
        vj = v_ref[j * per : (j + 1) * per].reshape(KC, HEAD)
        dp = dot(vj, gT)
        pb = p_ref[rows, :]
        ds = (pb.astype(F32) * (dp - delta)).astype(BF16)
        dv_ref[rows, :] += dot(pb, g)
        dk_ref[rows, :] += dot(ds, qn)
        dqT = dqT + dot(knT_ref[:, rows], ds)
    dq = dqT.T * SCALE
    grad, part = norm_back(dq, raw, qgain)
    gq_ref[...] += part
    return out, grad


def local_kernel(
    spans_ref, in_ref, pos_ref, qgain_ref, kgain_ref, out_ref, gains_ref,
    kn_ref, knT_ref, vT_ref, kpos_ref, limit_ref, s_ref, p_ref, dk_ref, dv_ref, gq_ref,
):
    q_ref, k_ref, v_ref, do_ref = (in_ref.at[i] for i in range(4))
    qgain, kgain = qgain_ref[...], kgain_ref[...]
    spans = [
        (spans_ref[0, i].astype(F32), (spans_ref[0, i] + spans_ref[1, i]).astype(F32))
        for i in range(2)
    ]
    place_masks(pos_ref, spans, kpos_ref, limit_ref)
    prepare_keys(k_ref, v_ref, kgain, kn_ref, knT_ref, vT_ref)
    dk_ref[...] = jnp.zeros_like(dk_ref)
    dv_ref[...] = jnp.zeros_like(dv_ref)
    gq_ref[...] = jnp.zeros_like(gq_ref)

    @pl.loop(0, STEPS)
    def _(b):
        out, grad = query_step(
            b, q_ref, do_ref, v_ref, qgain, kn_ref, knT_ref, vT_ref, kpos_ref, limit_ref,
            s_ref, p_ref, dk_ref, dv_ref, gq_ref,
        )
        out_ref[0, pl.ds(b * PER, PER)] = out.reshape(PER, TOK, HEAD)
        out_ref[1, pl.ds(b * PER, PER)] = grad.reshape(PER, TOK, HEAD)

    gk = jnp.zeros((1, HEAD), F32)
    for r in range(MEMBERS):
        rows = slice(r * TOK, (r + 1) * TOK)
        grad, part = norm_back(dk_ref[rows, :] * SCALE, k_ref[r], kgain)
        gk = gk + part
        out_ref[2, r] = grad
        out_ref[3, r] = dv_ref[rows, :].astype(BF16)
    gains_ref[0:1, :] = gq_ref[...]
    gains_ref[1:2, :] = gk


def local_call(spans, packed, places, qgain, kgain):
    vmem = pl.BlockSpec(memory_space=pltpu.VMEM)
    return pl.pallas_call(
        local_kernel,
        out_shape=(
            jax.ShapeDtypeStruct((4, MEMBERS, TOK, HEAD), BF16),
            jax.ShapeDtypeStruct((2, HEAD), F32),
        ),
        in_specs=[pl.BlockSpec(memory_space=pltpu.SMEM)] + [vmem] * 4,
        out_specs=(vmem, vmem),
        scratch_shapes=[
            pltpu.VMEM((LEN, HEAD), BF16),
            pltpu.VMEM((HEAD, LEN), BF16),
            pltpu.VMEM((HEAD, LEN), BF16),
            pltpu.VMEM((LEN, 128), F32),
            pltpu.VMEM((STEPS, 1, QB), F32),
            pltpu.VMEM((LEN, QB), F32),
            pltpu.VMEM((LEN, QB), BF16),
            pltpu.VMEM((LEN, HEAD), F32),
            pltpu.VMEM((LEN, HEAD), F32),
            pltpu.VMEM((1, HEAD), F32),
        ],
        compiler_params=pltpu.CompilerParams(vmem_limit_bytes=40 << 20),
    )(spans, packed, places, qgain, kgain)


def body(query_rows, key_rows, value_rows, cotangent, query_gain, key_gain, positions, span_start, span_length):
    rows = query_rows.shape[0]
    core = lax.axis_index("ctx_2")
    head = lax.axis_index(PEERS)
    packed = jnp.stack(
        [t.reshape(rows, HEADS, HEAD).transpose(1, 0, 2) for t in (query_rows, key_rows, value_rows, cotangent)],
        axis=0,
    )
    packed = lax.all_to_all(packed, PEERS, split_axis=1, concat_axis=1, tiled=True)
    places = lax.all_gather(positions, PEERS).astype(F32)
    spans = jnp.stack(
        [lax.dynamic_index_in_dim(t, core, 0, keepdims=False) for t in (span_start, span_length)]
    )
    pick = lambda g: lax.dynamic_index_in_dim(g.reshape(HEADS, HEAD), head, 0, keepdims=True)
    outs, gains = local_call(spans, packed, places, pick(query_gain), pick(key_gain))
    outs = lax.all_to_all(outs, PEERS, split_axis=1, concat_axis=1, tiled=True)
    outs = [outs[i].transpose(1, 0, 2).reshape(rows, HEADS * HEAD) for i in range(4)]
    slots = (jnp.arange(HEADS) == head)[None, :, None]
    gain_grads = jnp.where(slots, gains[:, None, :], 0.0).reshape(2, HEADS * HEAD)
    gain_grads = lax.psum(gain_grads, DP_CTX)
    return (*outs, gain_grads)


def solution(mesh):
    split = Mesh(mesh.devices.reshape(2, 4, 2, 8, 2), DP_CTX)
    rows = P(DP_CTX, None)
    return jax.shard_map(
        body,
        mesh=split,
        in_specs=(rows, rows, rows, rows, P(), P(), P(DP_CTX), P(DP, None), P(DP, None)),
        out_specs=(rows, rows, rows, rows, P()),
        check_vma=False,
    )
```

```python
import jax
import jax.numpy as jnp
from jax import lax
from jax.experimental import pallas as pl
from jax.experimental.pallas import tpu as pltpu
from jax.sharding import Mesh
from jax.sharding import PartitionSpec as P

HEADS = 16
HEAD = 128
DP_CTX = ("dp_0", "dp_1", "ctx_0", "ctx_1", "ctx_2")
DP = ("dp_0", "dp_1")
EPS = 1e-05
MASKED = -1e30
SCALE = HEAD**-0.5
LOG2E = 1.4426950408889634
MESH = pl.DeviceIdType.MESH
F32 = jnp.float32
BF16 = jnp.bfloat16

TOK = 128
MEMBERS = 16
LEN = TOK * MEMBERS
PER = 2
QB = TOK * PER
STEPS = MEMBERS // PER
KC = 256
CHUNKS = LEN // KC


def unit_of(raw):
    values = raw.astype(F32)
    inverse = lax.rsqrt(jnp.mean(values * values, axis=-1, keepdims=True) + EPS)
    return values * inverse, inverse


def norm_back(grad, raw, gain):
    unit, inverse = unit_of(raw)
    u = grad * gain
    projected = jnp.mean(u * unit, axis=-1, keepdims=True)
    part = jnp.sum(grad * unit, axis=0, keepdims=True)
    return (inverse * (u - unit * projected)).astype(BF16), part


def dot(a, b):
    return jnp.dot(a, b, preferred_element_type=F32)


def fold8(x, op):
    return op(x.reshape(x.shape[0] // 8, 8, x.shape[1]), axis=0)


def prepare_key(n, k_ref, kgain, kn_ref, knT_ref):
    rows = pl.ds(pl.multiple_of(n * TOK, TOK), TOK)
    unit, _ = unit_of(k_ref[n])
    normed = unit * kgain
    kn_ref[rows, :] = normed.astype(BF16)
    knT_ref[:, rows] = normed.T.astype(BF16)


def prepare_value(n, v_ref, vT_ref):
    rows = pl.ds(pl.multiple_of(n * TOK, TOK), TOK)
    vT_ref[:, rows] = v_ref[n].astype(F32).T.astype(BF16)


def query_step(
    b, q_ref, do_ref, v_ref, qgain, kn_ref, knT_ref, vT_ref, kpos_ref, limit_ref, s_ref, p_ref, dk_ref, dv_ref, gq_ref
):
    raw = q_ref[pl.ds(b * PER, PER)].reshape(QB, HEAD)
    unit, _ = unit_of(raw)
    normed = unit * qgain
    qn = normed.astype(BF16)
    qnT = normed.T.astype(BF16)
    limit = limit_ref[b]
    top = jnp.full((8, QB), MASKED, F32)
    for j in range(CHUNKS):
        rows = slice(j * KC, (j + 1) * KC)
        kp = kpos_ref[rows, :]
        kp = jnp.concatenate([kp] * (QB // 128), axis=1)
        s = jnp.where(kp < limit, dot(kn_ref[rows, :], qnT) * (SCALE * LOG2E), MASKED)
        s_ref[rows, :] = s
        top = jnp.maximum(top, fold8(s, jnp.max))
    top = jnp.max(top, axis=0, keepdims=True)
    total = jnp.zeros((8, QB), F32)
    oT = jnp.zeros((HEAD, QB), F32)
    for j in range(CHUNKS):
        rows = slice(j * KC, (j + 1) * KC)
        p = jnp.exp2(s_ref[rows, :] - top)
        total = total + fold8(p, jnp.sum)
        pb = p.astype(BF16)
        p_ref[rows, :] = pb
        oT = oT + dot(vT_ref[:, rows], pb)
    inv = 1.0 / jnp.sum(total, axis=0, keepdims=True)
    oT = (oT * inv).astype(BF16).astype(F32)
    out = oT.T.astype(BF16)
    gradT = do_ref[pl.ds(b * PER, PER)].reshape(QB, HEAD).astype(F32).T * inv
    gT = gradT.astype(BF16)
    gT32 = gT.astype(F32)
    g = gT32.T.astype(BF16)
    delta = jnp.sum(oT * gT32, axis=0, keepdims=True)
    dqT = jnp.zeros((HEAD, QB), F32)
    for j in range(CHUNKS):
        rows = slice(j * KC, (j + 1) * KC)
        per = KC // TOK
        vj = v_ref[j * per : (j + 1) * per].reshape(KC, HEAD)
        dp = dot(vj, gT)
        pb = p_ref[rows, :]
        ds = (pb.astype(F32) * (dp - delta)).astype(BF16)
        dv_ref[rows, :] += dot(pb, g)
        dk_ref[rows, :] += dot(ds, qn)
        dqT = dqT + dot(knT_ref[:, rows], ds)
    dq = dqT.T * SCALE
    grad, part = norm_back(dq, raw, qgain)
    gq_ref[...] += part
    return out, grad


def across(step):
    return lax.rem(8 + lax.div(step + 1, 2) * (2 * lax.rem(step, 2) - 1), 8)


def device(y, z):
    return {"ctx_0": y, "ctx_1": z}


def columns(head):
    return pl.ds(pl.multiple_of(head * HEAD, HEAD), HEAD)


def fused_kernel(
    start_ref, length_ref, q_hbm, k_hbm, v_hbm, do_hbm, place_ref, qgain_ref, kgain_ref,
    out_hbm, gq_hbm, gk_hbm, gv_hbm, gains_ref,
    recv, places, send, kn_ref, knT_ref, vT_ref, kpos_ref, limit_ref, s_ref, p_ref, dk_ref, dv_ref, gq_ref,
    part_ref, parts, whole_ref, wholes, in_send, in_recv, back_send, back_recv, gain_send, gain_recv,
):
    y, z, core = lax.axis_index("ctx_0"), lax.axis_index("ctx_1"), lax.axis_index("ctx_2")
    d0, d1 = lax.axis_index("dp_0"), lax.axis_index("dp_1")
    me = y * 8 + z
    member = d0 * 8 + d1 * 2 + core

    def target(n):
        return lax.rem(y + lax.rem(n, 2), 2), lax.rem(z + across(lax.div(n, 2)), 8)

    def origin(n):
        return lax.rem(y + lax.rem(n, 2), 2), lax.rem(z + 8 - across(lax.div(n, 2)), 8)

    def sibling(t):
        return {
            "dp_0": lax.rem(d0 + t // 8, 2),
            "dp_1": lax.rem(d1 + t // 2 % 4, 4),
            "ctx_2": lax.rem(core + t % 2, 2),
        }

    targets = [target(jnp.int32(n)) for n in range(MEMBERS)]
    barrier = pltpu.get_barrier_semaphore()
    for n in range(1, MEMBERS):
        pl.semaphore_signal(barrier, inc=1, device_id=device(*targets[n]), device_id_type=MESH)
        pl.semaphore_signal(barrier, inc=1, device_id=sibling(n), device_id_type=MESH)
    pl.semaphore_wait(barrier, 2 * (MEMBERS - 1))

    def incoming(a, n, at):
        if a == 4:
            source, dest = place_ref, places.at[n]
        else:
            source, dest = (q_hbm, k_hbm, v_hbm, do_hbm)[a], recv.at[a, n]
            source = source.at[:, columns(at[0] * 8 + at[1])]
        return source, dest

    def arrival(a, n, at):
        source, dest = incoming(a, n, at)
        return pltpu.make_async_remote_copy(
            source, dest, in_send.at[a, n], in_recv.at[a, n], device_id=device(*at), device_id_type=MESH
        )

    def own(a):
        source, dest = incoming(a, 0, (y, z))
        return pltpu.make_async_copy(source, dest, in_recv.at[a, 0])

    for group in ((4,), (1,), (2,), (0, 3)):
        for a in group:
            own(a).start()
        for n in range(1, MEMBERS):
            for a in group:
                arrival(a, n, targets[n]).start()

    qgain, kgain = qgain_ref[pl.ds(me, 1), :], kgain_ref[pl.ds(me, 1), :]
    dk_ref[...] = jnp.zeros_like(dk_ref)
    dv_ref[...] = jnp.zeros_like(dv_ref)
    gq_ref[...] = jnp.zeros_like(gq_ref)
    part_ref[...] = jnp.zeros_like(part_ref)
    spans = []
    for i in range(2):
        first = start_ref[core, i]
        spans.append((first.astype(F32), (first + length_ref[core, i]).astype(F32)))

    own(4).wait()
    for n in range(1, MEMBERS):
        arrival(4, n, targets[n]).wait_recv()
    for n in range(MEMBERS):
        row = places[n]
        limit = row + 1.0
        for start, end in spans:
            limit = jnp.where((row >= start) & (row < end), end, limit)
        limit_ref[n // PER, :, n % PER * TOK : (n % PER + 1) * TOK] = limit
        kpos_ref[n * TOK : (n + 1) * TOK, :] = jnp.broadcast_to(row, (TOK, TOK)).T

    own(1).wait()
    prepare_key(0, recv.at[1], kgain, kn_ref, knT_ref)

    @pl.loop(1, MEMBERS)
    def _(n):
        arrival(1, n, (y, z)).wait_recv()
        prepare_key(n, recv.at[1], kgain, kn_ref, knT_ref)

    own(2).wait()
    prepare_value(0, recv.at[2], vT_ref)

    @pl.loop(1, MEMBERS)
    def _(n):
        arrival(2, n, (y, z)).wait_recv()
        prepare_value(n, recv.at[2], vT_ref)

    outs = (out_hbm, gq_hbm, gk_hbm, gv_hbm)

    def back(i, n, at, head):
        return pltpu.make_async_remote_copy(
            send.at[i, n], outs[i].at[:, columns(head)], back_send.at[i, n], back_recv.at[i, n],
            device_id=device(*at), device_id_type=MESH,
        )

    def stays(i):
        return pltpu.make_async_copy(send.at[i, 0], outs[i].at[:, columns(me)], back_send.at[i, 0])

    def send_step(b):
        for j in range(PER):
            n = b * PER + j
            if j == 0:

                @pl.when(b == 0)
                def _():
                    stays(0).start()
                    stays(1).start()

                @pl.when(b > 0)
                def _():
                    back(0, n, origin(n), me).start()
                    back(1, n, origin(n), me).start()

            else:
                back(0, n, origin(n), me).start()
                back(1, n, origin(n), me).start()

    own(0).wait()
    own(3).wait()

    @pl.loop(0, STEPS)
    def _(b):
        @pl.when(b > 0)
        def _():
            arrival(0, b * PER, (y, z)).wait_recv()
            arrival(3, b * PER, (y, z)).wait_recv()

        for j in range(1, PER):
            arrival(0, b * PER + j, (y, z)).wait_recv()
            arrival(3, b * PER + j, (y, z)).wait_recv()
        out, grad = query_step(
            b, recv.at[0], recv.at[3], recv.at[2], qgain, kn_ref, knT_ref, vT_ref, kpos_ref, limit_ref,
            s_ref, p_ref, dk_ref, dv_ref, gq_ref,
        )
        send[0, pl.ds(b * PER, PER)] = out.reshape(PER, TOK, HEAD)
        send[1, pl.ds(b * PER, PER)] = grad.reshape(PER, TOK, HEAD)

        @pl.when(b > 0)
        def _():
            send_step(b - 1)

    for n in range(MEMBERS):
        send[3, n] = dv_ref[n * TOK : (n + 1) * TOK, :].astype(BF16)
    send_step(jnp.int32(STEPS - 1))
    gk = jnp.zeros((1, HEAD), F32)
    for n in range(MEMBERS):
        grad, part = norm_back(dk_ref[n * TOK : (n + 1) * TOK, :] * SCALE, recv[1, n], kgain)
        gk = gk + part
        send[2, n] = grad
        if n == 0:
            part_ref[0:1, :] = gq_ref[...]
            stays(3).start()
        else:
            back(3, n, origin(jnp.int32(n)), me).start()
    part_ref[1:2, :] = gk
    parts[member] = part_ref[...]

    def half(n):
        if n == 0:
            stays(2).start()
        else:
            back(2, n, origin(jnp.int32(n)), me).start()

    def spread(t):
        return pltpu.make_async_remote_copy(
            part_ref, parts.at[member], gain_send.at[0, t], gain_recv.at[0, t],
            device_id=sibling(t), device_id_type=MESH,
        )

    def publish(n):
        return pltpu.make_async_remote_copy(
            whole_ref, wholes.at[me], gain_send.at[1, n], gain_recv.at[1, n],
            device_id=device(*targets[n]), device_id_type=MESH,
        )

    for n in range(4):
        half(n)
    for t in range(1, MEMBERS):
        spread(t).start()
    for n in range(4, 8):
        half(n)
    for t in range(1, MEMBERS):
        spread(t).wait_recv()
    whole = parts[0]
    for t in range(1, MEMBERS):
        whole = whole + parts[t]
    whole_ref[...] = whole
    wholes[me] = whole
    for n in range(8, 12):
        half(n)
    for n in range(1, MEMBERS):
        publish(n).start()
    for n in range(12, MEMBERS):
        half(n)
    for n in range(1, MEMBERS):
        publish(n).wait_recv()
    for h in range(HEADS):
        gains_ref[:, h * HEAD : (h + 1) * HEAD] = wholes[h, 0:2, :]

    for n in range(1, MEMBERS):
        spread(n).wait_send()
        publish(n).wait_send()
        for a in range(5):
            arrival(a, n, targets[n]).wait_send()
    for i in range(4):
        stays(i).wait()
    for n in range(1, MEMBERS):
        yy, zz = targets[n]
        for i in range(4):
            back(i, n, (yy, zz), yy * 8 + zz).wait()


def body(query_rows, key_rows, value_rows, cotangent, query_gain, key_gain, positions, span_start, span_length):
    rows = query_rows.shape[0]
    vmem = pl.BlockSpec(memory_space=pltpu.VMEM)
    smem = pl.BlockSpec(memory_space=pltpu.SMEM)
    hbm = pl.BlockSpec(memory_space=pl.ANY)
    row_array = jax.ShapeDtypeStruct((rows, HEADS * HEAD), BF16)
    dma = pltpu.SemaphoreType.DMA
    return pl.pallas_call(
        fused_kernel,
        out_shape=(row_array,) * 4 + (jax.ShapeDtypeStruct((2, HEADS * HEAD), F32),),
        in_specs=[smem] * 2 + [hbm] * 4 + [vmem] * 3,
        out_specs=(hbm,) * 4 + (vmem,),
        scratch_shapes=[
            pltpu.VMEM((4, MEMBERS, TOK, HEAD), BF16),
            pltpu.VMEM((MEMBERS, 1, TOK), F32),
            pltpu.VMEM((4, MEMBERS, TOK, HEAD), BF16),
            pltpu.VMEM((LEN, HEAD), BF16),
            pltpu.VMEM((HEAD, LEN), BF16),
            pltpu.VMEM((HEAD, LEN), BF16),
            pltpu.VMEM((LEN, 128), F32),
            pltpu.VMEM((STEPS, 1, QB), F32),
            pltpu.VMEM((LEN, QB), F32),
            pltpu.VMEM((LEN, QB), BF16),
            pltpu.VMEM((LEN, HEAD), F32),
            pltpu.VMEM((LEN, HEAD), F32),
            pltpu.VMEM((1, HEAD), F32),
            pltpu.VMEM((8, HEAD), F32),
            pltpu.VMEM((MEMBERS, 8, HEAD), F32),
            pltpu.VMEM((8, HEAD), F32),
            pltpu.VMEM((MEMBERS, 8, HEAD), F32),
            dma((5, MEMBERS)),
            dma((5, MEMBERS)),
            dma((4, MEMBERS)),
            dma((4, MEMBERS)),
            dma((2, MEMBERS)),
            dma((2, MEMBERS)),
        ],
        compiler_params=pltpu.CompilerParams(
            collective_id=0, has_side_effects=True, vmem_limit_bytes=40 << 20
        ),
    )(
        span_start, span_length, query_rows, key_rows, value_rows, cotangent,
        positions.astype(F32).reshape(1, TOK), query_gain.reshape(HEADS, HEAD), key_gain.reshape(HEADS, HEAD),
    )


def solution(mesh):
    split = Mesh(mesh.devices.reshape(2, 4, 2, 8, 2), DP_CTX)
    rows = P(DP_CTX, None)
    return jax.shard_map(
        body,
        mesh=split,
        in_specs=(rows, rows, rows, rows, P(), P(), P(DP_CTX), P(DP, None), P(DP, None)),
        out_specs=(rows, rows, rows, rows, P()),
        check_vma=False,
    )
```

```python
import jax
import jax.numpy as jnp
from jax import lax
from jax.experimental import pallas as pl
from jax.experimental.pallas import tpu as pltpu
from jax.sharding import Mesh
from jax.sharding import PartitionSpec as P

HEADS = 16
HEAD = 128
DP_CTX = ("dp_0", "dp_1", "ctx_0", "ctx_1", "ctx_2")
DP = ("dp_0", "dp_1")
EPS = 1e-05
MASKED = -1e30
SCALE = HEAD**-0.5
LOG2E = 1.4426950408889634
MESH = pl.DeviceIdType.MESH
F32 = jnp.float32
BF16 = jnp.bfloat16

SEQS = 2
SPANS = 2
TOK = 128
MEMBERS = 16
LEN = TOK * MEMBERS
PER = 2
QB = TOK * PER
STEPS = MEMBERS // PER
KC = 256
CHUNKS = LEN // KC
GRANT = 40 << 20


def unit_of(raw):
    values = raw.astype(F32)
    inverse = lax.rsqrt(jnp.mean(values * values, axis=-1, keepdims=True) + EPS)
    return values * inverse, inverse


def norm_back(grad, raw, gain):
    unit, inverse = unit_of(raw)
    u = grad * gain
    projected = jnp.mean(u * unit, axis=-1, keepdims=True)
    part = jnp.sum(grad * unit, axis=0, keepdims=True)
    return (inverse * (u - unit * projected)).astype(BF16), part


def dot(a, b):
    return jnp.dot(a, b, preferred_element_type=F32)


def fold8(x, op):
    return op(x.reshape(x.shape[0] // 8, 8, x.shape[1]), axis=0)


def prepare_key(n, k_ref, kgain, kn_ref, knT_ref):
    rows = pl.ds(pl.multiple_of(n * TOK, TOK), TOK)
    unit, _ = unit_of(k_ref[n])
    normed = unit * kgain
    kn_ref[rows, :] = normed.astype(BF16)
    knT_ref[:, rows] = normed.T.astype(BF16)


def prepare_value(n, v_ref, vT_ref):
    rows = pl.ds(pl.multiple_of(n * TOK, TOK), TOK)
    vT_ref[:, rows] = v_ref[n].astype(F32).T.astype(BF16)


def query_step(
    b, q_ref, do_ref, v_ref, qgain, kn_ref, knT_ref, vT_ref, kpos_ref, limit_ref, s_ref, p_ref, dk_ref, dv_ref, gq_ref
):
    raw = q_ref[pl.ds(b * PER, PER)].reshape(QB, HEAD)
    unit, _ = unit_of(raw)
    normed = unit * qgain
    qn = normed.astype(BF16)
    qnT = normed.T.astype(BF16)
    limit = limit_ref[b]
    top = jnp.full((8, QB), MASKED, F32)
    for j in range(CHUNKS):
        rows = slice(j * KC, (j + 1) * KC)
        kp = kpos_ref[rows, :]
        kp = jnp.concatenate([kp] * (QB // 128), axis=1)
        s = jnp.where(kp < limit, dot(kn_ref[rows, :], qnT) * (SCALE * LOG2E), MASKED)
        s_ref[rows, :] = s
        top = jnp.maximum(top, fold8(s, jnp.max))
    top = jnp.max(top, axis=0, keepdims=True)
    total = jnp.zeros((8, QB), F32)
    oT = jnp.zeros((HEAD, QB), F32)
    for j in range(CHUNKS):
        rows = slice(j * KC, (j + 1) * KC)
        p = jnp.exp2(s_ref[rows, :] - top)
        total = total + fold8(p, jnp.sum)
        pb = p.astype(BF16)
        p_ref[rows, :] = pb
        oT = oT + dot(vT_ref[:, rows], pb)
    inv = 1.0 / jnp.sum(total, axis=0, keepdims=True)
    oT = (oT * inv).astype(BF16).astype(F32)
    out = oT.T.astype(BF16)
    gradT = do_ref[pl.ds(b * PER, PER)].reshape(QB, HEAD).astype(F32).T * inv
    gT = gradT.astype(BF16)
    gT32 = gT.astype(F32)
    g = gT32.T.astype(BF16)
    delta = jnp.sum(oT * gT32, axis=0, keepdims=True)
    dqT = jnp.zeros((HEAD, QB), F32)
    for j in range(CHUNKS):
        rows = slice(j * KC, (j + 1) * KC)
        per = KC // TOK
        vj = v_ref[j * per : (j + 1) * per].reshape(KC, HEAD)
        dp = dot(vj, gT)
        pb = p_ref[rows, :]
        ds = (pb.astype(F32) * (dp - delta)).astype(BF16)
        dv_ref[rows, :] += dot(pb, g)
        dk_ref[rows, :] += dot(ds, qn)
        dqT = dqT + dot(knT_ref[:, rows], ds)
    dq = dqT.T * SCALE
    grad, part = norm_back(dq, raw, qgain)
    gq_ref[...] += part
    return out, grad


def across(step):
    return lax.rem(8 + lax.div(step + 1, 2) * (2 * lax.rem(step, 2) - 1), 8)


def device(y, z):
    return {"ctx_0": y, "ctx_1": z}


def columns(head):
    return pl.ds(pl.multiple_of(head * HEAD, HEAD), HEAD)


def fused_kernel(
    start_hbm, length_hbm, q_hbm, k_hbm, v_hbm, do_hbm, place_ref, qgain_hbm, kgain_hbm,
    out_hbm, gq_hbm, gk_hbm, gv_hbm, gains_ref,
    recv, places, send, kn_ref, knT_ref, vT_ref, kpos_ref, limit_ref, s_ref, p_ref, dk_ref, dv_ref, gq_ref,
    part_ref, parts, whole_ref, wholes, start_ref, length_ref, qgain_ref, kgain_ref, small, in_send, in_recv, back_send, back_recv, gain_send, gain_recv,
):
    y, z, core = lax.axis_index("ctx_0"), lax.axis_index("ctx_1"), lax.axis_index("ctx_2")
    d0, d1 = lax.axis_index("dp_0"), lax.axis_index("dp_1")
    me = y * 8 + z
    member = d0 * 8 + d1 * 2 + core

    def target(n):
        return lax.rem(y + lax.rem(n, 2), 2), lax.rem(z + across(lax.div(n, 2)), 8)

    def origin(n):
        return lax.rem(y + lax.rem(n, 2), 2), lax.rem(z + 8 - across(lax.div(n, 2)), 8)

    def sibling(t):
        return {
            "dp_0": lax.rem(d0 + t // 8, 2),
            "dp_1": lax.rem(d1 + t // 2 % 4, 4),
            "ctx_2": lax.rem(core + t % 2, 2),
        }

    targets = [target(jnp.int32(n)) for n in range(MEMBERS)]
    barrier = pltpu.get_barrier_semaphore()
    for n in range(1, MEMBERS):
        pl.semaphore_signal(barrier, inc=1, device_id=device(*targets[n]), device_id_type=MESH)
        pl.semaphore_signal(barrier, inc=1, device_id=sibling(n), device_id_type=MESH)
    fetches = [
        pltpu.make_async_copy(source, dest, small.at[i])
        for i, (source, dest) in enumerate(
            (
                (start_hbm, start_ref),
                (length_hbm, length_ref),
                (qgain_hbm.at[pl.ds(me, 1), :], qgain_ref),
                (kgain_hbm.at[pl.ds(me, 1), :], kgain_ref),
            )
        )
    ]
    for fetch in fetches:
        fetch.start()
    dk_ref[...] = jnp.zeros_like(dk_ref)
    dv_ref[...] = jnp.zeros_like(dv_ref)
    gq_ref[...] = jnp.zeros_like(gq_ref)
    part_ref[...] = jnp.zeros_like(part_ref)
    pl.semaphore_wait(barrier, 2 * (MEMBERS - 1))

    def incoming(a, n, at):
        if a == 4:
            source, dest = place_ref, places.at[n]
        else:
            source, dest = (q_hbm, k_hbm, v_hbm, do_hbm)[a], recv.at[a, n]
            source = source.at[:, columns(at[0] * 8 + at[1])]
        return source, dest

    def arrival(a, n, at):
        source, dest = incoming(a, n, at)
        return pltpu.make_async_remote_copy(
            source, dest, in_send.at[a, n], in_recv.at[a, n], device_id=device(*at), device_id_type=MESH
        )

    def own(a):
        source, dest = incoming(a, 0, (y, z))
        return pltpu.make_async_copy(source, dest, in_recv.at[a, 0])

    for group in ((4,), (1,), (2,), (0, 3)):
        for a in group:
            own(a).start()
        for n in range(1, MEMBERS):
            for a in group:
                arrival(a, n, targets[n]).start()

    for fetch in fetches:
        fetch.wait()
    qgain, kgain = qgain_ref[...], kgain_ref[...]
    spans = []
    for i in range(2):
        first = start_ref[core, i]
        spans.append((first.astype(F32), (first + length_ref[core, i]).astype(F32)))

    own(4).wait()
    for n in range(1, MEMBERS):
        arrival(4, n, targets[n]).wait_recv()
    for n in range(MEMBERS):
        row = places[n].astype(F32)
        limit = row + 1.0
        for start, end in spans:
            limit = jnp.where((row >= start) & (row < end), end, limit)
        limit_ref[n // PER, :, n % PER * TOK : (n % PER + 1) * TOK] = limit
        kpos_ref[n * TOK : (n + 1) * TOK, :] = jnp.broadcast_to(row, (TOK, TOK)).T

    own(1).wait()
    prepare_key(0, recv.at[1], kgain, kn_ref, knT_ref)

    @pl.loop(1, MEMBERS)
    def _(n):
        arrival(1, n, (y, z)).wait_recv()
        prepare_key(n, recv.at[1], kgain, kn_ref, knT_ref)

    own(2).wait()
    prepare_value(0, recv.at[2], vT_ref)

    @pl.loop(1, MEMBERS)
    def _(n):
        arrival(2, n, (y, z)).wait_recv()
        prepare_value(n, recv.at[2], vT_ref)

    outs = (out_hbm, gq_hbm, gk_hbm, gv_hbm)

    def back(i, n, at, head):
        return pltpu.make_async_remote_copy(
            send.at[i, n], outs[i].at[:, columns(head)], back_send.at[i, n], back_recv.at[i, n],
            device_id=device(*at), device_id_type=MESH,
        )

    def stays(i):
        return pltpu.make_async_copy(send.at[i, 0], outs[i].at[:, columns(me)], back_send.at[i, 0])

    def send_step(b):
        for j in range(PER):
            n = b * PER + j
            if j == 0:

                @pl.when(b == 0)
                def _():
                    stays(0).start()
                    stays(1).start()

                @pl.when(b > 0)
                def _():
                    back(0, n, origin(n), me).start()
                    back(1, n, origin(n), me).start()

            else:
                back(0, n, origin(n), me).start()
                back(1, n, origin(n), me).start()

    own(0).wait()
    own(3).wait()

    @pl.loop(0, STEPS)
    def _(b):
        @pl.when(b > 0)
        def _():
            arrival(0, b * PER, (y, z)).wait_recv()
            arrival(3, b * PER, (y, z)).wait_recv()

        for j in range(1, PER):
            arrival(0, b * PER + j, (y, z)).wait_recv()
            arrival(3, b * PER + j, (y, z)).wait_recv()
        out, grad = query_step(
            b, recv.at[0], recv.at[3], recv.at[2], qgain, kn_ref, knT_ref, vT_ref, kpos_ref, limit_ref,
            s_ref, p_ref, dk_ref, dv_ref, gq_ref,
        )
        send[0, pl.ds(b * PER, PER)] = out.reshape(PER, TOK, HEAD)
        send[1, pl.ds(b * PER, PER)] = grad.reshape(PER, TOK, HEAD)

        @pl.when(b > 0)
        def _():
            send_step(b - 1)

    for n in range(MEMBERS):
        send[3, n] = dv_ref[n * TOK : (n + 1) * TOK, :].astype(BF16)
    send_step(jnp.int32(STEPS - 1))
    gk = jnp.zeros((1, HEAD), F32)
    for n in range(MEMBERS):
        grad, part = norm_back(dk_ref[n * TOK : (n + 1) * TOK, :] * SCALE, recv[1, n], kgain)
        gk = gk + part
        send[2, n] = grad
        if n == 0:
            part_ref[0:1, :] = gq_ref[...]
            stays(3).start()
        else:
            back(3, n, origin(jnp.int32(n)), me).start()
    part_ref[1:2, :] = gk
    parts[member] = part_ref[...]

    def half(n):
        if n == 0:
            stays(2).start()
        else:
            back(2, n, origin(jnp.int32(n)), me).start()

    def spread(t):
        return pltpu.make_async_remote_copy(
            part_ref, parts.at[member], gain_send.at[0, t], gain_recv.at[0, t],
            device_id=sibling(t), device_id_type=MESH,
        )

    def publish(n):
        return pltpu.make_async_remote_copy(
            whole_ref, wholes.at[me], gain_send.at[1, n], gain_recv.at[1, n],
            device_id=device(*targets[n]), device_id_type=MESH,
        )

    for n in range(4):
        half(n)
    for t in range(1, MEMBERS):
        spread(t).start()
    for n in range(4, 8):
        half(n)
    for t in range(1, MEMBERS):
        spread(t).wait_recv()
    whole = parts[0]
    for t in range(1, MEMBERS):
        whole = whole + parts[t]
    whole_ref[...] = whole
    wholes[me] = whole
    for n in range(8, 12):
        half(n)
    for n in range(1, MEMBERS):
        publish(n).start()
    for n in range(12, MEMBERS):
        half(n)
    for n in range(1, MEMBERS):
        publish(n).wait_recv()
    for h in range(HEADS):
        gains_ref[:, h * HEAD : (h + 1) * HEAD] = wholes[h, 0:2, :]

    for n in range(1, MEMBERS):
        spread(n).wait_send()
        publish(n).wait_send()
        for a in range(5):
            arrival(a, n, targets[n]).wait_send()
    for i in range(4):
        stays(i).wait()
    for n in range(1, MEMBERS):
        yy, zz = targets[n]
        for i in range(4):
            back(i, n, (yy, zz), yy * 8 + zz).wait()


def hand_over(*refs):
    sems = refs[-1]
    copies = [pltpu.make_async_copy(refs[i], refs[5 + i], sems.at[i]) for i in range(5)]
    for copy in copies:
        copy.start()
    for copy in copies:
        copy.wait()


def body(query_rows, key_rows, value_rows, cotangent, query_gain, key_gain, positions, span_start, span_length):
    rows = query_rows.shape[0]
    vmem = pl.BlockSpec(memory_space=pltpu.VMEM)
    hbm = pl.BlockSpec(memory_space=pltpu.HBM)
    free = pl.BlockSpec(memory_space=pl.ANY)
    row_array = jax.ShapeDtypeStruct((rows, HEADS * HEAD), BF16)
    dma = pltpu.SemaphoreType.DMA
    results = row_array, row_array, row_array, row_array, jax.ShapeDtypeStruct((2, HEADS * HEAD), F32)
    landed = pl.pallas_call(
        fused_kernel,
        out_shape=results,
        in_specs=[hbm] * 9,
        out_specs=(free,) * 4 + (vmem,),
        scratch_shapes=[
            pltpu.VMEM((4, MEMBERS, TOK, HEAD), BF16),
            pltpu.VMEM((MEMBERS, 1, TOK), jnp.int32),
            pltpu.VMEM((4, MEMBERS, TOK, HEAD), BF16),
            pltpu.VMEM((LEN, HEAD), BF16),
            pltpu.VMEM((HEAD, LEN), BF16),
            pltpu.VMEM((HEAD, LEN), BF16),
            pltpu.VMEM((LEN, 128), F32),
            pltpu.VMEM((STEPS, 1, QB), F32),
            pltpu.VMEM((LEN, QB), F32),
            pltpu.VMEM((LEN, QB), BF16),
            pltpu.VMEM((LEN, HEAD), F32),
            pltpu.VMEM((LEN, HEAD), F32),
            pltpu.VMEM((1, HEAD), F32),
            pltpu.VMEM((8, HEAD), F32),
            pltpu.VMEM((MEMBERS, 8, HEAD), F32),
            pltpu.VMEM((8, HEAD), F32),
            pltpu.VMEM((MEMBERS, 8, HEAD), F32),
            pltpu.SMEM((SEQS, SPANS), jnp.int32),
            pltpu.SMEM((SEQS, SPANS), jnp.int32),
            pltpu.VMEM((1, HEAD), F32),
            pltpu.VMEM((1, HEAD), F32),
            dma((4,)),
            dma((5, MEMBERS)),
            dma((5, MEMBERS)),
            dma((4, MEMBERS)),
            dma((4, MEMBERS)),
            dma((2, MEMBERS)),
            dma((2, MEMBERS)),
        ],
        compiler_params=pltpu.CompilerParams(
            collective_id=0, has_side_effects=True, vmem_limit_bytes=GRANT
        ),
    )(
        *(
            pltpu.with_memory_space_constraint(t, pltpu.HBM)
            for t in (
                span_start, span_length, query_rows, key_rows, value_rows, cotangent,
                positions.reshape(1, TOK), query_gain.reshape(HEADS, HEAD), key_gain.reshape(HEADS, HEAD),
            )
        )
    )
    return pl.pallas_call(
        hand_over,
        out_shape=results,
        in_specs=[free] * 5,
        out_specs=(hbm,) * 5,
        scratch_shapes=[dma((5,))],
        compiler_params=pltpu.CompilerParams(vmem_limit_bytes=1 << 20),
    )(*landed)


def solution(mesh):
    split = Mesh(mesh.devices.reshape(2, 4, 2, 8, 2), DP_CTX)
    rows = P(DP_CTX, None)
    return jax.shard_map(
        body,
        mesh=split,
        in_specs=(rows, rows, rows, rows, P(), P(), P(DP_CTX), P(DP, None), P(DP, None)),
        out_specs=(rows, rows, rows, rows, P()),
        check_vma=False,
    )
```

```python
import jax
import jax.numpy as jnp
from jax import lax
from jax.experimental import pallas as pl
from jax.experimental.pallas import tpu as pltpu
from jax.sharding import Mesh
from jax.sharding import PartitionSpec as P

HEADS = 16
HEAD = 128
DP_CTX = ("dp_0", "dp_1", "ctx_0", "ctx_1", "ctx_2")
DP = ("dp_0", "dp_1")
EPS = 1e-05
MASKED = -1e30
SCALE = HEAD**-0.5
LOG2E = 1.4426950408889634
MESH = pl.DeviceIdType.MESH
F32 = jnp.float32
BF16 = jnp.bfloat16

SEQS = 2
SPANS = 2
TOK = 128
MEMBERS = 16
LEN = TOK * MEMBERS
PER = 2
QB = TOK * PER
STEPS = MEMBERS // PER
KC = 256
CHUNKS = LEN // KC
GRANT = 40 << 20
HELD = 8


def unit_of(raw):
    values = raw.astype(F32)
    inverse = lax.rsqrt(jnp.mean(values * values, axis=-1, keepdims=True) + EPS)
    return values * inverse, inverse


def norm_back(grad, raw, gain):
    unit, inverse = unit_of(raw)
    u = grad * gain
    projected = jnp.mean(u * unit, axis=-1, keepdims=True)
    part = jnp.sum(grad * unit, axis=0, keepdims=True)
    return (inverse * (u - unit * projected)).astype(BF16), part


def dot(a, b):
    return jnp.dot(a, b, preferred_element_type=F32)


def fold8(x, op):
    return op(x.reshape(x.shape[0] // 8, 8, x.shape[1]), axis=0)


def prepare_key(n, k_ref, kgain, kn_ref, knT_ref):
    rows = pl.ds(pl.multiple_of(n * TOK, TOK), TOK)
    unit, _ = unit_of(k_ref[n])
    normed = unit * kgain
    kn_ref[rows, :] = normed.astype(BF16)
    knT_ref[:, rows] = normed.T.astype(BF16)


def prepare_value(n, v_ref, vT_ref):
    rows = pl.ds(pl.multiple_of(n * TOK, TOK), TOK)
    vT_ref[:, rows] = v_ref[n].astype(F32).T.astype(BF16)


def query_step(
    b, q_ref, do_ref, v_ref, qgain, kn_ref, knT_ref, vT_ref, kpos_ref, limit_ref, s_ref, p_ref, dk_ref, dv_ref, gq_ref
):
    raw = q_ref[pl.ds(b * PER, PER)].reshape(QB, HEAD)
    unit, _ = unit_of(raw)
    normed = unit * qgain
    qn = normed.astype(BF16)
    qnT = normed.T.astype(BF16)
    limit = limit_ref[b]
    top = jnp.full((8, QB), MASKED, F32)
    for j in range(CHUNKS):
        rows = slice(j * KC, (j + 1) * KC)
        kp = kpos_ref[rows, :]
        kp = jnp.concatenate([kp] * (QB // 128), axis=1)
        s = jnp.where(kp < limit, dot(kn_ref[rows, :], qnT) * (SCALE * LOG2E), MASKED)
        s_ref[rows, :] = s
        top = jnp.maximum(top, fold8(s, jnp.max))
    top = jnp.max(top, axis=0, keepdims=True)
    total = jnp.zeros((8, QB), F32)
    oT = jnp.zeros((HEAD, QB), F32)
    for j in range(CHUNKS):
        rows = slice(j * KC, (j + 1) * KC)
        p = jnp.exp2(s_ref[rows, :] - top)
        total = total + fold8(p, jnp.sum)
        pb = p.astype(BF16)
        p_ref[rows, :] = pb
        oT = oT + dot(vT_ref[:, rows], pb)
    inv = 1.0 / jnp.sum(total, axis=0, keepdims=True)
    oT = (oT * inv).astype(BF16).astype(F32)
    out = oT.T.astype(BF16)
    gradT = do_ref[pl.ds(b * PER, PER)].reshape(QB, HEAD).astype(F32).T * inv
    gT = gradT.astype(BF16)
    gT32 = gT.astype(F32)
    g = gT32.T.astype(BF16)
    delta = jnp.sum(oT * gT32, axis=0, keepdims=True)
    dqT = jnp.zeros((HEAD, QB), F32)
    for j in range(CHUNKS):
        rows = slice(j * KC, (j + 1) * KC)
        per = KC // TOK
        vj = v_ref[j * per : (j + 1) * per].reshape(KC, HEAD)
        dp = dot(vj, gT)
        pb = p_ref[rows, :]
        ds = (pb.astype(F32) * (dp - delta)).astype(BF16)
        dv_ref[rows, :] += dot(pb, g)
        dk_ref[rows, :] += dot(ds, qn)
        dqT = dqT + dot(knT_ref[:, rows], ds)
    dq = dqT.T * SCALE
    grad, part = norm_back(dq, raw, qgain)
    gq_ref[...] += part
    return out, grad


def across(step):
    return lax.rem(8 + lax.div(step + 1, 2) * (2 * lax.rem(step, 2) - 1), 8)


def device(y, z):
    return {"ctx_0": y, "ctx_1": z}


def columns(head):
    return pl.ds(pl.multiple_of(head * HEAD, HEAD), HEAD)


def fused_kernel(
    start_hbm, length_hbm, q_hbm, k_hbm, v_hbm, do_hbm, place_ref, qgain_hbm, kgain_hbm,
    out_hbm, gq_hbm, gk_hbm, gv_hbm, gains_ref,
    recv, places, send, kn_ref, knT_ref, vT_ref, kpos_ref, limit_ref, s_ref, p_ref, dk_ref, dv_ref, gq_ref,
    sums, others, wholes, start_ref, length_ref, qgain_ref, kgain_ref, small, in_send, in_recv, back_send, back_recv,
    pair_send, pair_recv, gain_send, gain_recv, rounds,
):
    y, z, core = lax.axis_index("ctx_0"), lax.axis_index("ctx_1"), lax.axis_index("ctx_2")
    d0, d1 = lax.axis_index("dp_0"), lax.axis_index("dp_1")
    me = y * 8 + z

    def target(n):
        return lax.rem(y + lax.rem(n, 2), 2), lax.rem(z + across(lax.div(n, 2)), 8)

    def origin(n):
        return lax.rem(y + lax.rem(n, 2), 2), lax.rem(z + 8 - across(lax.div(n, 2)), 8)

    kin = (
        {"ctx_2": 1 - core},
        {"dp_1": d1 + 1 - 2 * lax.rem(d1, 2)},
        {"dp_1": 3 - d1},
        {"dp_0": 1 - d0},
    )
    targets = [target(jnp.int32(n)) for n in range(MEMBERS)]
    sides = [device(*targets[2]), device(*targets[4])]
    barrier = pltpu.get_barrier_semaphore()
    for at in (*sides, device(*targets[1]), *kin):
        pl.semaphore_signal(barrier, inc=1, device_id=at, device_id_type=MESH)

    def incoming(a, n, at):
        if a == 4:
            source, dest = place_ref, places.at[n]
        else:
            source, dest = (q_hbm, k_hbm, v_hbm, do_hbm)[a], recv.at[a, n]
            source = source.at[:, columns(at[0] * 8 + at[1])]
        return source, dest

    def arrival(a, n, at):
        source, dest = incoming(a, n, at)
        return pltpu.make_async_remote_copy(
            source, dest, in_send.at[a, n], in_recv.at[a, n], device_id=device(*at), device_id_type=MESH
        )

    def own(a):
        source, dest = incoming(a, 0, (y, z))
        return pltpu.make_async_copy(source, dest, in_recv.at[a, 0])

    for a in (4, 1, 2, 0, 3):
        own(a).start()
    fetches = [
        pltpu.make_async_copy(source, dest, small.at[i])
        for i, (source, dest) in enumerate(
            (
                (start_hbm, start_ref),
                (length_hbm, length_ref),
                (qgain_hbm.at[pl.ds(me, 1), :], qgain_ref),
                (kgain_hbm.at[pl.ds(me, 1), :], kgain_ref),
            )
        )
    ]
    for fetch in fetches:
        fetch.start()
    pl.semaphore_wait(barrier, 3 + len(kin))

    for r, known in enumerate(((1, 2, 4), (3, 5, 6, 8), (7, 9, 10, 12), (11, 13, 14), (15,))):
        if r > 0:
            pl.semaphore_wait(rounds.at[r - 1], 2)
        if r < 4:
            for at in sides:
                pl.semaphore_signal(rounds.at[r], inc=1, device_id=at, device_id_type=MESH)
        for n in known:
            for a in (4, 1, 2):
                arrival(a, n, targets[n]).start()
    for n in range(1, MEMBERS):
        for a in (0, 3):
            arrival(a, n, targets[n]).start()

    dk_ref[...] = jnp.zeros_like(dk_ref)
    dv_ref[...] = jnp.zeros_like(dv_ref)
    gq_ref[...] = jnp.zeros_like(gq_ref)
    for fetch in fetches:
        fetch.wait()
    qgain, kgain = qgain_ref[...], kgain_ref[...]
    spans = []
    for i in range(2):
        first = start_ref[core, i]
        spans.append((first.astype(F32), (first + length_ref[core, i]).astype(F32)))

    own(4).wait()
    for n in range(1, MEMBERS):
        arrival(4, n, targets[n]).wait_recv()
    for n in range(MEMBERS):
        row = places[n].astype(F32)
        limit = row + 1.0
        for start, end in spans:
            limit = jnp.where((row >= start) & (row < end), end, limit)
        limit_ref[n // PER, :, n % PER * TOK : (n % PER + 1) * TOK] = limit
        kpos_ref[n * TOK : (n + 1) * TOK, :] = jnp.broadcast_to(row, (TOK, TOK)).T

    own(1).wait()
    prepare_key(0, recv.at[1], kgain, kn_ref, knT_ref)

    @pl.loop(1, MEMBERS)
    def _(n):
        arrival(1, n, (y, z)).wait_recv()
        prepare_key(n, recv.at[1], kgain, kn_ref, knT_ref)

    own(2).wait()
    prepare_value(0, recv.at[2], vT_ref)

    @pl.loop(1, MEMBERS)
    def _(n):
        arrival(2, n, (y, z)).wait_recv()
        prepare_value(n, recv.at[2], vT_ref)

    outs = (out_hbm, gq_hbm, gk_hbm, gv_hbm)

    def back(i, n, at, head):
        return pltpu.make_async_remote_copy(
            send.at[i, n], outs[i].at[:, columns(head)], back_send.at[i, n], back_recv.at[i, n],
            device_id=device(*at), device_id_type=MESH,
        )

    def stays(i):
        return pltpu.make_async_copy(send.at[i, 0], outs[i].at[:, columns(me)], back_send.at[i, 0])

    def send_step(b):
        for j in range(PER):
            n = b * PER + j
            if j == 0:

                @pl.when(b == 0)
                def _():
                    stays(0).start()
                    stays(1).start()

                @pl.when(b > 0)
                def _():
                    back(0, n, origin(n), me).start()
                    back(1, n, origin(n), me).start()

            else:
                back(0, n, origin(n), me).start()
                back(1, n, origin(n), me).start()

    own(0).wait()
    own(3).wait()

    @pl.loop(0, STEPS)
    def _(b):
        @pl.when(b > 0)
        def _():
            arrival(0, b * PER, (y, z)).wait_recv()
            arrival(3, b * PER, (y, z)).wait_recv()

        for j in range(1, PER):
            arrival(0, b * PER + j, (y, z)).wait_recv()
            arrival(3, b * PER + j, (y, z)).wait_recv()
        out, grad = query_step(
            b, recv.at[0], recv.at[3], recv.at[2], qgain, kn_ref, knT_ref, vT_ref, kpos_ref, limit_ref,
            s_ref, p_ref, dk_ref, dv_ref, gq_ref,
        )
        send[0, pl.ds(b * PER, PER)] = out.reshape(PER, TOK, HEAD)
        send[1, pl.ds(b * PER, PER)] = grad.reshape(PER, TOK, HEAD)

        @pl.when(b > 0)
        def _():
            send_step(b - 1)

    def results(i, n):
        if n == 0:
            stays(i).start()
        else:
            back(i, n, origin(jnp.int32(n)), me).start()

    def exchange(e):
        return pltpu.make_async_remote_copy(
            sums.at[e], others.at[e], pair_send.at[e], pair_recv.at[e], device_id=kin[e], device_id_type=MESH
        )

    def publish(n):
        return pltpu.make_async_remote_copy(
            sums.at[len(kin)], wholes.at[me], gain_send.at[n], gain_recv.at[n],
            device_id=device(*targets[n]), device_id_type=MESH,
        )

    send_step(jnp.int32(STEPS - 1))
    gk = jnp.zeros((1, HEAD), F32)
    for n in range(MEMBERS):
        grad, part = norm_back(dk_ref[n * TOK : (n + 1) * TOK, :] * SCALE, recv[1, n], kgain)
        gk = gk + part
        send[2, n] = grad
    sums[0] = jnp.concatenate([gq_ref[...], gk, jnp.zeros((6, HEAD), F32)], axis=0)
    for n in range(MEMBERS):
        send[3, n] = dv_ref[n * TOK : (n + 1) * TOK, :].astype(BF16)
    for e in range(len(kin)):
        exchange(e).start()
        if e == len(kin) - 1:
            for n in range(3 * e, MEMBERS):
                results(3, n)
            for n in range(MEMBERS - HELD):
                results(2, n)
        exchange(e).wait_recv()
        sums[e + 1] = sums[e] + others[e]
        if e < len(kin) - 1:
            for n in range(3 * e, 3 * e + 3):
                results(3, n)
    wholes[me] = sums[len(kin)]
    for n in range(MEMBERS - HELD, MEMBERS - HELD + 2):
        results(2, n)
    for n in range(1, MEMBERS):
        publish(n).start()
    for n in range(MEMBERS - HELD + 2, MEMBERS):
        results(2, n)
    for n in range(1, MEMBERS):
        publish(n).wait_recv()
    for h in range(HEADS):
        gains_ref[:, h * HEAD : (h + 1) * HEAD] = wholes[h, 0:2, :]

    for n in range(1, MEMBERS):
        publish(n).wait_send()
        for a in range(5):
            arrival(a, n, targets[n]).wait_send()
    for e in range(len(kin)):
        exchange(e).wait_send()
    for i in range(4):
        stays(i).wait()
    for n in range(1, MEMBERS):
        yy, zz = targets[n]
        for i in range(4):
            back(i, n, (yy, zz), yy * 8 + zz).wait()


def hand_over(*refs):
    sems = refs[-1]
    copies = [pltpu.make_async_copy(refs[i], refs[5 + i], sems.at[i]) for i in range(5)]
    for copy in copies:
        copy.start()
    for copy in copies:
        copy.wait()


def body(query_rows, key_rows, value_rows, cotangent, query_gain, key_gain, positions, span_start, span_length):
    rows = query_rows.shape[0]
    vmem = pl.BlockSpec(memory_space=pltpu.VMEM)
    hbm = pl.BlockSpec(memory_space=pltpu.HBM)
    free = pl.BlockSpec(memory_space=pl.ANY)
    row_array = jax.ShapeDtypeStruct((rows, HEADS * HEAD), BF16)
    dma = pltpu.SemaphoreType.DMA
    results = row_array, row_array, row_array, row_array, jax.ShapeDtypeStruct((2, HEADS * HEAD), F32)
    landed = pl.pallas_call(
        fused_kernel,
        out_shape=results,
        in_specs=[hbm] * 9,
        out_specs=(free,) * 4 + (vmem,),
        scratch_shapes=[
            pltpu.VMEM((4, MEMBERS, TOK, HEAD), BF16),
            pltpu.VMEM((MEMBERS, 1, TOK), jnp.int32),
            pltpu.VMEM((4, MEMBERS, TOK, HEAD), BF16),
            pltpu.VMEM((LEN, HEAD), BF16),
            pltpu.VMEM((HEAD, LEN), BF16),
            pltpu.VMEM((HEAD, LEN), BF16),
            pltpu.VMEM((LEN, 128), F32),
            pltpu.VMEM((STEPS, 1, QB), F32),
            pltpu.VMEM((LEN, QB), F32),
            pltpu.VMEM((LEN, QB), BF16),
            pltpu.VMEM((LEN, HEAD), F32),
            pltpu.VMEM((LEN, HEAD), F32),
            pltpu.VMEM((1, HEAD), F32),
            pltpu.VMEM((5, 8, HEAD), F32),
            pltpu.VMEM((4, 8, HEAD), F32),
            pltpu.VMEM((MEMBERS, 8, HEAD), F32),
            pltpu.SMEM((SEQS, SPANS), jnp.int32),
            pltpu.SMEM((SEQS, SPANS), jnp.int32),
            pltpu.VMEM((1, HEAD), F32),
            pltpu.VMEM((1, HEAD), F32),
            dma((4,)),
            dma((5, MEMBERS)),
            dma((5, MEMBERS)),
            dma((4, MEMBERS)),
            dma((4, MEMBERS)),
            dma((4,)),
            dma((4,)),
            dma((MEMBERS,)),
            dma((MEMBERS,)),
            pltpu.SemaphoreType.REGULAR((4,)),
        ],
        compiler_params=pltpu.CompilerParams(
            collective_id=0, has_side_effects=True, vmem_limit_bytes=GRANT
        ),
    )(
        *(
            pltpu.with_memory_space_constraint(t, pltpu.HBM)
            for t in (
                span_start, span_length, query_rows, key_rows, value_rows, cotangent,
                positions.reshape(1, TOK), query_gain.reshape(HEADS, HEAD), key_gain.reshape(HEADS, HEAD),
            )
        )
    )
    return pl.pallas_call(
        hand_over,
        out_shape=results,
        in_specs=[free] * 5,
        out_specs=(hbm,) * 5,
        scratch_shapes=[dma((5,))],
        compiler_params=pltpu.CompilerParams(vmem_limit_bytes=1 << 20),
    )(*landed)


def solution(mesh):
    split = Mesh(mesh.devices.reshape(2, 4, 2, 8, 2), DP_CTX)
    rows = P(DP_CTX, None)
    return jax.shard_map(
        body,
        mesh=split,
        in_specs=(rows, rows, rows, rows, P(), P(), P(DP_CTX), P(DP, None), P(DP, None)),
        out_specs=(rows, rows, rows, rows, P()),
        check_vma=False,
    )
```

```python
import jax
import jax.numpy as jnp
from jax import lax
from jax.experimental import pallas as pl
from jax.experimental.pallas import tpu as pltpu
from jax.sharding import Mesh
from jax.sharding import PartitionSpec as P

HEADS = 16
HEAD = 128
DP_CTX = ("dp_0", "dp_1", "ctx_0", "ctx_1", "ctx_2")
DP = ("dp_0", "dp_1")
EPS = 1e-05
MASKED = -1e30
SCALE = HEAD**-0.5
LOG2E = 1.4426950408889634
MESH = pl.DeviceIdType.MESH
F32 = jnp.float32
BF16 = jnp.bfloat16

SEQS = 2
SPANS = 2
TOK = 128
MEMBERS = 16
LEN = TOK * MEMBERS
PER = 2
QB = TOK * PER
STEPS = MEMBERS // PER
KC = 256
CHUNKS = LEN // KC
GRANT = 40 << 20
HELD = 8


def unit_of(raw):
    values = raw.astype(F32)
    inverse = lax.rsqrt(jnp.mean(values * values, axis=-1, keepdims=True) + EPS)
    return values * inverse, inverse


def norm_back(grad, raw, gain):
    unit, inverse = unit_of(raw)
    u = grad * gain
    projected = jnp.mean(u * unit, axis=-1, keepdims=True)
    part = jnp.sum(grad * unit, axis=0, keepdims=True)
    return (inverse * (u - unit * projected)).astype(BF16), part


def dot(a, b):
    return jnp.dot(a, b, preferred_element_type=F32)


def fold8(x, op):
    return op(x.reshape(x.shape[0] // 8, 8, x.shape[1]), axis=0)


def prepare_key(n, k_ref, kgain, kn_ref, knT_ref):
    rows = pl.ds(pl.multiple_of(n * TOK, TOK), TOK)
    unit, _ = unit_of(k_ref[n])
    normed = unit * kgain
    kn_ref[rows, :] = normed.astype(BF16)
    knT_ref[:, rows] = normed.T.astype(BF16)


def prepare_value(n, v_ref, vT_ref):
    rows = pl.ds(pl.multiple_of(n * TOK, TOK), TOK)
    vT_ref[:, rows] = v_ref[n].astype(F32).T.astype(BF16)


def query_step(
    b, q_ref, do_ref, v_ref, qgain, kn_ref, knT_ref, vT_ref, kpos_ref, limit_ref, s_ref, p_ref, dk_ref, dv_ref, gq_ref
):
    raw = q_ref[pl.ds(b * PER, PER)].reshape(QB, HEAD)
    unit, _ = unit_of(raw)
    normed = unit * qgain
    qn = normed.astype(BF16)
    qnT = normed.T.astype(BF16)
    limit = limit_ref[b]
    top = jnp.full((8, QB), MASKED, F32)
    for j in range(CHUNKS):
        rows = slice(j * KC, (j + 1) * KC)
        kp = kpos_ref[rows, :]
        kp = jnp.concatenate([kp] * (QB // 128), axis=1)
        s = jnp.where(kp < limit, dot(kn_ref[rows, :], qnT) * (SCALE * LOG2E), MASKED)
        s_ref[rows, :] = s
        top = jnp.maximum(top, fold8(s, jnp.max))
    top = jnp.max(top, axis=0, keepdims=True)
    total = jnp.zeros((8, QB), F32)
    for j in range(CHUNKS):
        rows = slice(j * KC, (j + 1) * KC)
        total = total + fold8(jnp.exp2(s_ref[rows, :] - top), jnp.sum)
    top = top + jnp.log2(jnp.sum(total, axis=0, keepdims=True))
    oT = jnp.zeros((HEAD, QB), F32)
    for j in range(CHUNKS):
        rows = slice(j * KC, (j + 1) * KC)
        p = jnp.exp2(s_ref[rows, :] - top)
        s_ref[rows, :] = p
        weights = p.astype(BF16)
        p_ref[rows, :] = weights
        oT = oT + dot(vT_ref[:, rows], weights)
    oT = oT.astype(BF16).astype(F32)
    out = oT.T.astype(BF16)
    g = do_ref[pl.ds(b * PER, PER)].reshape(QB, HEAD)
    gT32 = g.astype(F32).T
    gT = gT32.astype(BF16)
    delta = jnp.sum(oT * gT32, axis=0, keepdims=True)
    dqT = jnp.zeros((HEAD, QB), F32)
    for j in range(CHUNKS):
        rows = slice(j * KC, (j + 1) * KC)
        per = KC // TOK
        vj = v_ref[j * per : (j + 1) * per].reshape(KC, HEAD)
        ds = (s_ref[rows, :] * (dot(vj, gT) - delta)).astype(BF16)
        dv_ref[rows, :] += dot(p_ref[rows, :], g)
        dk_ref[rows, :] += dot(ds, qn)
        dqT = dqT + dot(knT_ref[:, rows], ds)
    dq = dqT.T * SCALE
    grad, part = norm_back(dq, raw, qgain)
    gq_ref[...] += part
    return out, grad


def across(step):
    return lax.rem(8 + lax.div(step + 1, 2) * (2 * lax.rem(step, 2) - 1), 8)


def device(y, z):
    return {"ctx_0": y, "ctx_1": z}


def columns(head):
    return pl.ds(pl.multiple_of(head * HEAD, HEAD), HEAD)


def fused_kernel(
    start_hbm, length_hbm, q_hbm, k_hbm, v_hbm, do_hbm, place_ref, qgain_hbm, kgain_hbm,
    out_hbm, gq_hbm, gk_hbm, gv_hbm, gains_ref,
    recv, places, send, kn_ref, knT_ref, vT_ref, kpos_ref, limit_ref, s_ref, p_ref, dk_ref, dv_ref, gq_ref,
    sums, others, wholes, start_ref, length_ref, qgain_ref, kgain_ref, small, in_send, in_recv, back_send, back_recv,
    pair_send, pair_recv, gain_send, gain_recv, rounds,
):
    y, z, core = lax.axis_index("ctx_0"), lax.axis_index("ctx_1"), lax.axis_index("ctx_2")
    d0, d1 = lax.axis_index("dp_0"), lax.axis_index("dp_1")
    me = y * 8 + z

    def target(n):
        return lax.rem(y + lax.rem(n, 2), 2), lax.rem(z + across(lax.div(n, 2)), 8)

    def origin(n):
        return lax.rem(y + lax.rem(n, 2), 2), lax.rem(z + 8 - across(lax.div(n, 2)), 8)

    kin = (
        {"ctx_2": 1 - core},
        {"dp_1": d1 + 1 - 2 * lax.rem(d1, 2)},
        {"dp_1": 3 - d1},
        {"dp_0": 1 - d0},
    )
    targets = [target(jnp.int32(n)) for n in range(MEMBERS)]
    sides = [device(*targets[2]), device(*targets[4])]
    barrier = pltpu.get_barrier_semaphore()
    for at in (*sides, device(*targets[1]), *kin):
        pl.semaphore_signal(barrier, inc=1, device_id=at, device_id_type=MESH)

    def incoming(a, n, at):
        if a == 4:
            source, dest = place_ref, places.at[n]
        else:
            source, dest = (q_hbm, k_hbm, v_hbm, do_hbm)[a], recv.at[a, n]
            source = source.at[:, columns(at[0] * 8 + at[1])]
        return source, dest

    def arrival(a, n, at):
        source, dest = incoming(a, n, at)
        return pltpu.make_async_remote_copy(
            source, dest, in_send.at[a, n], in_recv.at[a, n], device_id=device(*at), device_id_type=MESH
        )

    def own(a):
        source, dest = incoming(a, 0, (y, z))
        return pltpu.make_async_copy(source, dest, in_recv.at[a, 0])

    for a in (4, 1, 2, 0, 3):
        own(a).start()
    fetches = [
        pltpu.make_async_copy(source, dest, small.at[i])
        for i, (source, dest) in enumerate(
            (
                (start_hbm, start_ref),
                (length_hbm, length_ref),
                (qgain_hbm.at[pl.ds(me, 1), :], qgain_ref),
                (kgain_hbm.at[pl.ds(me, 1), :], kgain_ref),
            )
        )
    ]
    for fetch in fetches:
        fetch.start()
    pl.semaphore_wait(barrier, 3 + len(kin))

    for r, known in enumerate(((1, 2, 4), (3, 5, 6, 8), (7, 9, 10, 12), (11, 13, 14), (15,))):
        if r > 0:
            pl.semaphore_wait(rounds.at[r - 1], 2)
        if r < 4:
            for at in sides:
                pl.semaphore_signal(rounds.at[r], inc=1, device_id=at, device_id_type=MESH)
        for n in known:
            for a in (4, 1, 2):
                arrival(a, n, targets[n]).start()
    for n in range(1, MEMBERS):
        for a in (0, 3):
            arrival(a, n, targets[n]).start()

    dk_ref[...] = jnp.zeros_like(dk_ref)
    dv_ref[...] = jnp.zeros_like(dv_ref)
    gq_ref[...] = jnp.zeros_like(gq_ref)
    for fetch in fetches:
        fetch.wait()
    qgain, kgain = qgain_ref[...], kgain_ref[...]
    spans = []
    for i in range(2):
        first = start_ref[core, i]
        spans.append((first.astype(F32), (first + length_ref[core, i]).astype(F32)))

    own(4).wait()
    for n in range(1, MEMBERS):
        arrival(4, n, targets[n]).wait_recv()
    for n in range(MEMBERS):
        row = places[n].astype(F32)
        limit = row + 1.0
        for start, end in spans:
            limit = jnp.where((row >= start) & (row < end), end, limit)
        limit_ref[n // PER, :, n % PER * TOK : (n % PER + 1) * TOK] = limit
        kpos_ref[n * TOK : (n + 1) * TOK, :] = jnp.broadcast_to(row, (TOK, TOK)).T

    own(1).wait()
    prepare_key(0, recv.at[1], kgain, kn_ref, knT_ref)

    @pl.loop(1, MEMBERS)
    def _(n):
        arrival(1, n, (y, z)).wait_recv()
        prepare_key(n, recv.at[1], kgain, kn_ref, knT_ref)

    own(2).wait()
    prepare_value(0, recv.at[2], vT_ref)

    @pl.loop(1, MEMBERS)
    def _(n):
        arrival(2, n, (y, z)).wait_recv()
        prepare_value(n, recv.at[2], vT_ref)

    outs = (out_hbm, gq_hbm, gk_hbm, gv_hbm)

    def back(i, n, at, head):
        return pltpu.make_async_remote_copy(
            send.at[i, n], outs[i].at[:, columns(head)], back_send.at[i, n], back_recv.at[i, n],
            device_id=device(*at), device_id_type=MESH,
        )

    def stays(i):
        return pltpu.make_async_copy(send.at[i, 0], outs[i].at[:, columns(me)], back_send.at[i, 0])

    def send_step(b):
        for j in range(PER):
            n = b * PER + j
            if j == 0:

                @pl.when(b == 0)
                def _():
                    stays(0).start()
                    stays(1).start()

                @pl.when(b > 0)
                def _():
                    back(0, n, origin(n), me).start()
                    back(1, n, origin(n), me).start()

            else:
                back(0, n, origin(n), me).start()
                back(1, n, origin(n), me).start()

    own(0).wait()
    own(3).wait()

    @pl.loop(0, STEPS)
    def _(b):
        @pl.when(b > 0)
        def _():
            arrival(0, b * PER, (y, z)).wait_recv()
            arrival(3, b * PER, (y, z)).wait_recv()

        for j in range(1, PER):
            arrival(0, b * PER + j, (y, z)).wait_recv()
            arrival(3, b * PER + j, (y, z)).wait_recv()
        out, grad = query_step(
            b, recv.at[0], recv.at[3], recv.at[2], qgain, kn_ref, knT_ref, vT_ref, kpos_ref, limit_ref,
            s_ref, p_ref, dk_ref, dv_ref, gq_ref,
        )
        send[0, pl.ds(b * PER, PER)] = out.reshape(PER, TOK, HEAD)
        send[1, pl.ds(b * PER, PER)] = grad.reshape(PER, TOK, HEAD)

        @pl.when(b > 0)
        def _():
            send_step(b - 1)

    def results(i, n):
        if n == 0:
            stays(i).start()
        else:
            back(i, n, origin(jnp.int32(n)), me).start()

    def exchange(e):
        return pltpu.make_async_remote_copy(
            sums.at[e], others.at[e], pair_send.at[e], pair_recv.at[e], device_id=kin[e], device_id_type=MESH
        )

    def publish(n):
        return pltpu.make_async_remote_copy(
            sums.at[len(kin)], wholes.at[me], gain_send.at[n], gain_recv.at[n],
            device_id=device(*targets[n]), device_id_type=MESH,
        )

    gk = jnp.zeros((1, HEAD), F32)
    for n in range(MEMBERS):
        grad, part = norm_back(dk_ref[n * TOK : (n + 1) * TOK, :] * SCALE, recv[1, n], kgain)
        gk = gk + part
        send[2, n] = grad
    send_step(jnp.int32(STEPS - 1))
    sums[0] = jnp.concatenate([gq_ref[...], gk, jnp.zeros((6, HEAD), F32)], axis=0)
    for n in range(MEMBERS):
        send[3, n] = dv_ref[n * TOK : (n + 1) * TOK, :].astype(BF16)
    for e in range(len(kin)):
        exchange(e).start()
        if e == len(kin) - 1:
            for n in range(3 * e, MEMBERS):
                results(3, n)
            for n in range(MEMBERS - HELD):
                results(2, n)
        exchange(e).wait_recv()
        sums[e + 1] = sums[e] + others[e]
        if e < len(kin) - 1:
            for n in range(3 * e, 3 * e + 3):
                results(3, n)
    wholes[me] = sums[len(kin)]
    for n in range(MEMBERS - HELD, MEMBERS - HELD + 2):
        results(2, n)
    for n in range(1, MEMBERS):
        publish(n).start()
    for n in range(MEMBERS - HELD + 2, MEMBERS):
        results(2, n)
    for n in range(1, MEMBERS):
        publish(n).wait_recv()
    for h in range(HEADS):
        gains_ref[:, h * HEAD : (h + 1) * HEAD] = wholes[h, 0:2, :]

    for n in range(1, MEMBERS):
        publish(n).wait_send()
        for a in range(5):
            arrival(a, n, targets[n]).wait_send()
    for e in range(len(kin)):
        exchange(e).wait_send()
    for i in range(4):
        stays(i).wait()
    for n in range(1, MEMBERS):
        yy, zz = targets[n]
        for i in range(4):
            back(i, n, (yy, zz), yy * 8 + zz).wait()


def hand_over(*refs):
    sems = refs[-1]
    copies = [pltpu.make_async_copy(refs[i], refs[5 + i], sems.at[i]) for i in range(5)]
    for copy in copies:
        copy.start()
    for copy in copies:
        copy.wait()


def body(query_rows, key_rows, value_rows, cotangent, query_gain, key_gain, positions, span_start, span_length):
    rows = query_rows.shape[0]
    vmem = pl.BlockSpec(memory_space=pltpu.VMEM)
    hbm = pl.BlockSpec(memory_space=pltpu.HBM)
    free = pl.BlockSpec(memory_space=pl.ANY)
    row_array = jax.ShapeDtypeStruct((rows, HEADS * HEAD), BF16)
    dma = pltpu.SemaphoreType.DMA
    results = row_array, row_array, row_array, row_array, jax.ShapeDtypeStruct((2, HEADS * HEAD), F32)
    landed = pl.pallas_call(
        fused_kernel,
        out_shape=results,
        in_specs=[hbm] * 9,
        out_specs=(free,) * 4 + (vmem,),
        scratch_shapes=[
            pltpu.VMEM((4, MEMBERS, TOK, HEAD), BF16),
            pltpu.VMEM((MEMBERS, 1, TOK), jnp.int32),
            pltpu.VMEM((4, MEMBERS, TOK, HEAD), BF16),
            pltpu.VMEM((LEN, HEAD), BF16),
            pltpu.VMEM((HEAD, LEN), BF16),
            pltpu.VMEM((HEAD, LEN), BF16),
            pltpu.VMEM((LEN, 128), F32),
            pltpu.VMEM((STEPS, 1, QB), F32),
            pltpu.VMEM((LEN, QB), F32),
            pltpu.VMEM((LEN, QB), BF16),
            pltpu.VMEM((LEN, HEAD), F32),
            pltpu.VMEM((LEN, HEAD), F32),
            pltpu.VMEM((1, HEAD), F32),
            pltpu.VMEM((5, 8, HEAD), F32),
            pltpu.VMEM((4, 8, HEAD), F32),
            pltpu.VMEM((MEMBERS, 8, HEAD), F32),
            pltpu.SMEM((SEQS, SPANS), jnp.int32),
            pltpu.SMEM((SEQS, SPANS), jnp.int32),
            pltpu.VMEM((1, HEAD), F32),
            pltpu.VMEM((1, HEAD), F32),
            dma((4,)),
            dma((5, MEMBERS)),
            dma((5, MEMBERS)),
            dma((4, MEMBERS)),
            dma((4, MEMBERS)),
            dma((4,)),
            dma((4,)),
            dma((MEMBERS,)),
            dma((MEMBERS,)),
            pltpu.SemaphoreType.REGULAR((4,)),
        ],
        compiler_params=pltpu.CompilerParams(
            collective_id=0, has_side_effects=True, vmem_limit_bytes=GRANT
        ),
    )(
        *(
            pltpu.with_memory_space_constraint(t, pltpu.HBM)
            for t in (
                span_start, span_length, query_rows, key_rows, value_rows, cotangent,
                positions.reshape(1, TOK), query_gain.reshape(HEADS, HEAD), key_gain.reshape(HEADS, HEAD),
            )
        )
    )
    return pl.pallas_call(
        hand_over,
        out_shape=results,
        in_specs=[free] * 5,
        out_specs=(hbm,) * 5,
        scratch_shapes=[dma((5,))],
        compiler_params=pltpu.CompilerParams(vmem_limit_bytes=1 << 20),
    )(*landed)


def solution(mesh):
    split = Mesh(mesh.devices.reshape(2, 4, 2, 8, 2), DP_CTX)
    rows = P(DP_CTX, None)
    return jax.shard_map(
        body,
        mesh=split,
        in_specs=(rows, rows, rows, rows, P(), P(), P(DP_CTX), P(DP, None), P(DP, None)),
        out_specs=(rows, rows, rows, rows, P()),
        check_vma=False,
    )
```

```python
import jax
import jax.numpy as jnp
from jax import lax
from jax.experimental import pallas as pl
from jax.experimental.pallas import tpu as pltpu
from jax.sharding import Mesh
from jax.sharding import PartitionSpec as P

HEADS = 16
HEAD = 128
DP_CTX = ("dp_0", "dp_1", "ctx_0", "ctx_1", "ctx_2")
DP = ("dp_0", "dp_1")
EPS = 1e-05
MASKED = -1e30
SCALE = HEAD**-0.5
LOG2E = 1.4426950408889634
MESH = pl.DeviceIdType.MESH
F32 = jnp.float32
BF16 = jnp.bfloat16

SEQS = 2
SPANS = 2
TOK = 128
MEMBERS = 16
LEN = TOK * MEMBERS
PER = 2
QB = TOK * PER
STEPS = MEMBERS // PER
KC = 256
CHUNKS = LEN // KC
GRANT = 40 << 20
HELD = 8


def unit_of(raw):
    values = raw.astype(F32)
    inverse = lax.rsqrt(jnp.mean(values * values, axis=-1, keepdims=True) + EPS)
    return values * inverse, inverse


def norm_back(grad, raw, gain):
    unit, inverse = unit_of(raw)
    u = grad * gain
    projected = jnp.mean(u * unit, axis=-1, keepdims=True)
    part = jnp.sum(grad * unit, axis=0, keepdims=True)
    return (inverse * (u - unit * projected)).astype(BF16), part


def dot(a, b):
    return jnp.dot(a, b, preferred_element_type=F32)


def fold8(x, op):
    return op(x.reshape(x.shape[0] // 8, 8, x.shape[1]), axis=0)


def prepare_key(n, k_ref, kgain, kn_ref, knT_ref):
    rows = pl.ds(pl.multiple_of(n * TOK, TOK), TOK)
    unit, _ = unit_of(k_ref[n])
    normed = unit * kgain
    kn_ref[rows, :] = normed.astype(BF16)
    knT_ref[:, rows] = normed.T.astype(BF16)


def prepare_value(n, v_ref, vT_ref):
    rows = pl.ds(pl.multiple_of(n * TOK, TOK), TOK)
    vT_ref[:, rows] = v_ref[n].astype(F32).T.astype(BF16)


def query_step(
    b, q_ref, do_ref, v_ref, qgain, kn_ref, knT_ref, vT_ref, kpos_ref, limit_ref, s_ref, p_ref, dk_ref, dv_ref, gq_ref
):
    raw = q_ref[pl.ds(b * PER, PER)].reshape(QB, HEAD)
    unit, _ = unit_of(raw)
    normed = unit * qgain
    qn = normed.astype(BF16)
    qnT = normed.T.astype(BF16)
    limit = limit_ref[b]
    top = jnp.full((8, QB), MASKED, F32)
    for j in range(CHUNKS):
        rows = slice(j * KC, (j + 1) * KC)
        kp = kpos_ref[rows, :]
        kp = jnp.concatenate([kp] * (QB // 128), axis=1)
        s = jnp.where(kp < limit, dot(kn_ref[rows, :], qnT) * (SCALE * LOG2E), MASKED)
        s_ref[rows, :] = s
        top = jnp.maximum(top, fold8(s, jnp.max))
    top = jnp.max(top, axis=0, keepdims=True)
    total = jnp.zeros((8, QB), F32)
    for j in range(CHUNKS):
        rows = slice(j * KC, (j + 1) * KC)
        total = total + fold8(jnp.exp2(s_ref[rows, :] - top), jnp.sum)
    top = top + jnp.log2(jnp.sum(total, axis=0, keepdims=True))
    oT = jnp.zeros((HEAD, QB), F32)
    for j in range(CHUNKS):
        rows = slice(j * KC, (j + 1) * KC)
        p = jnp.exp2(s_ref[rows, :] - top)
        s_ref[rows, :] = p
        weights = p.astype(BF16)
        p_ref[rows, :] = weights
        oT = oT + dot(vT_ref[:, rows], weights)
    oT = oT.astype(BF16).astype(F32)
    out = oT.T.astype(BF16)
    g = do_ref[pl.ds(b * PER, PER)].reshape(QB, HEAD)
    gT32 = g.astype(F32).T
    gT = gT32.astype(BF16)
    delta = jnp.sum(oT * gT32, axis=0, keepdims=True)
    dqT = jnp.zeros((HEAD, QB), F32)
    for j in range(CHUNKS):
        rows = slice(j * KC, (j + 1) * KC)
        per = KC // TOK
        vj = v_ref[j * per : (j + 1) * per].reshape(KC, HEAD)
        ds = (s_ref[rows, :] * (dot(vj, gT) - delta)).astype(BF16)
        dv_ref[rows, :] += dot(p_ref[rows, :], g)
        dk_ref[rows, :] += dot(ds, qn)
        dqT = dqT + dot(knT_ref[:, rows], ds)
    dq = dqT.T * SCALE
    grad, part = norm_back(dq, raw, qgain)
    gq_ref[...] += part
    return out, grad


def across(step):
    return lax.rem(8 + lax.div(step + 1, 2) * (2 * lax.rem(step, 2) - 1), 8)


def device(y, z):
    return {"ctx_0": y, "ctx_1": z}


def columns(head):
    return pl.ds(pl.multiple_of(head * HEAD, HEAD), HEAD)


def fused_kernel(
    start_hbm, length_hbm, q_hbm, k_hbm, v_hbm, do_hbm, place_ref, qgain_hbm, kgain_hbm,
    out_hbm, gq_hbm, gk_hbm, gv_hbm, gains_ref,
    recv, places, send, kn_ref, knT_ref, vT_ref, kpos_ref, limit_ref, s_ref, p_ref, dk_ref, dv_ref, gq_ref,
    sums, others, wholes, start_ref, length_ref, qgain_ref, kgain_ref, small, in_send, in_recv, back_send, back_recv,
    pair_send, pair_recv, gain_send, gain_recv, rounds,
):
    y, z, core = lax.axis_index("ctx_0"), lax.axis_index("ctx_1"), lax.axis_index("ctx_2")
    d0, d1 = lax.axis_index("dp_0"), lax.axis_index("dp_1")
    me = y * 8 + z

    def target(n):
        return lax.rem(y + lax.rem(n, 2), 2), lax.rem(z + across(lax.div(n, 2)), 8)

    def origin(n):
        return lax.rem(y + lax.rem(n, 2), 2), lax.rem(z + 8 - across(lax.div(n, 2)), 8)

    kin = (
        {"ctx_2": 1 - core},
        {"dp_1": d1 + 1 - 2 * lax.rem(d1, 2)},
        {"dp_1": 3 - d1},
        {"dp_0": 1 - d0},
    )
    targets = [target(jnp.int32(n)) for n in range(MEMBERS)]
    sides = [device(*targets[2]), device(*targets[4])]
    barrier = pltpu.get_barrier_semaphore()
    for at in (*sides, device(*targets[1]), *kin):
        pl.semaphore_signal(barrier, inc=1, device_id=at, device_id_type=MESH)

    def incoming(a, n, at):
        if a == 4:
            source, dest = place_ref, places.at[n]
        else:
            source, dest = (q_hbm, k_hbm, v_hbm, do_hbm)[a], recv.at[a, n]
            source = source.at[:, columns(at[0] * 8 + at[1])]
        return source, dest

    def arrival(a, n, at):
        source, dest = incoming(a, n, at)
        return pltpu.make_async_remote_copy(
            source, dest, in_send.at[a, n], in_recv.at[a, n], device_id=device(*at), device_id_type=MESH
        )

    def own(a):
        source, dest = incoming(a, 0, (y, z))
        return pltpu.make_async_copy(source, dest, in_recv.at[a, 0])

    for a in (4, 1, 2, 0, 3):
        own(a).start()
    fetches = [
        pltpu.make_async_copy(source, dest, small.at[i])
        for i, (source, dest) in enumerate(
            (
                (start_hbm, start_ref),
                (length_hbm, length_ref),
                (qgain_hbm.at[pl.ds(me, 1), :], qgain_ref),
                (kgain_hbm.at[pl.ds(me, 1), :], kgain_ref),
            )
        )
    ]
    for fetch in fetches:
        fetch.start()
    pl.semaphore_wait(barrier, 3 + len(kin))

    for r, known in enumerate(((1, 2, 4), (3, 5, 6, 8), (7, 9, 10, 12), (11, 13, 14), (15,))):
        if r > 0:
            pl.semaphore_wait(rounds.at[r - 1], 2)
        if r < 4:
            for at in sides:
                pl.semaphore_signal(rounds.at[r], inc=1, device_id=at, device_id_type=MESH)
        for n in known:
            for a in (4, 1, 2):
                arrival(a, n, targets[n]).start()
    for n in range(1, MEMBERS):
        for a in (0, 3):
            arrival(a, n, targets[n]).start()

    dk_ref[...] = jnp.zeros_like(dk_ref)
    dv_ref[...] = jnp.zeros_like(dv_ref)
    gq_ref[...] = jnp.zeros_like(gq_ref)
    for fetch in fetches:
        fetch.wait()
    qgain, kgain = qgain_ref[...], kgain_ref[...]
    spans = []
    for i in range(2):
        first = start_ref[core, i]
        spans.append((first.astype(F32), (first + length_ref[core, i]).astype(F32)))

    own(4).wait()
    for n in range(1, MEMBERS):
        arrival(4, n, targets[n]).wait_recv()
    for n in range(MEMBERS):
        row = places[n].astype(F32)
        limit = row + 1.0
        for start, end in spans:
            limit = jnp.where((row >= start) & (row < end), end, limit)
        limit_ref[n // PER, :, n % PER * TOK : (n % PER + 1) * TOK] = limit
        kpos_ref[n * TOK : (n + 1) * TOK, :] = jnp.broadcast_to(row, (TOK, TOK)).T

    own(1).wait()
    prepare_key(0, recv.at[1], kgain, kn_ref, knT_ref)

    @pl.loop(1, MEMBERS)
    def _(n):
        arrival(1, n, (y, z)).wait_recv()
        prepare_key(n, recv.at[1], kgain, kn_ref, knT_ref)

    own(2).wait()
    prepare_value(0, recv.at[2], vT_ref)

    @pl.loop(1, MEMBERS)
    def _(n):
        arrival(2, n, (y, z)).wait_recv()
        prepare_value(n, recv.at[2], vT_ref)

    outs = (out_hbm, gq_hbm, gk_hbm, gv_hbm)

    def back(i, n, at, head):
        return pltpu.make_async_remote_copy(
            send.at[i, n], outs[i].at[:, columns(head)], back_send.at[i, n], back_recv.at[i, n],
            device_id=device(*at), device_id_type=MESH,
        )

    def stays(i):
        return pltpu.make_async_copy(send.at[i, 0], outs[i].at[:, columns(me)], back_send.at[i, 0])

    def send_step(b):
        for j in range(PER):
            n = b * PER + j
            if j == 0:

                @pl.when(b == 0)
                def _():
                    stays(0).start()
                    stays(1).start()

                @pl.when(b > 0)
                def _():
                    back(0, n, origin(n), me).start()
                    back(1, n, origin(n), me).start()

            else:
                back(0, n, origin(n), me).start()
                back(1, n, origin(n), me).start()

    own(0).wait()
    own(3).wait()

    @pl.loop(0, STEPS)
    def _(b):
        @pl.when(b > 0)
        def _():
            arrival(0, b * PER, (y, z)).wait_recv()
            arrival(3, b * PER, (y, z)).wait_recv()

        for j in range(1, PER):
            arrival(0, b * PER + j, (y, z)).wait_recv()
            arrival(3, b * PER + j, (y, z)).wait_recv()
        out, grad = query_step(
            b, recv.at[0], recv.at[3], recv.at[2], qgain, kn_ref, knT_ref, vT_ref, kpos_ref, limit_ref,
            s_ref, p_ref, dk_ref, dv_ref, gq_ref,
        )
        send[0, pl.ds(b * PER, PER)] = out.reshape(PER, TOK, HEAD)
        send[1, pl.ds(b * PER, PER)] = grad.reshape(PER, TOK, HEAD)

        @pl.when(b > 0)
        def _():
            send_step(b - 1)

    def results(i, n):
        if n == 0:
            stays(i).start()
        else:
            back(i, n, origin(jnp.int32(n)), me).start()

    def exchange(e):
        return pltpu.make_async_remote_copy(
            sums.at[e], others.at[e], pair_send.at[e], pair_recv.at[e], device_id=kin[e], device_id_type=MESH
        )

    def publish(n):
        return pltpu.make_async_remote_copy(
            sums.at[len(kin)], wholes.at[me], gain_send.at[n], gain_recv.at[n],
            device_id=device(*targets[n]), device_id_type=MESH,
        )

    gk = jnp.zeros((1, HEAD), F32)
    for n in range(MEMBERS):
        grad, part = norm_back(dk_ref[n * TOK : (n + 1) * TOK, :] * SCALE, recv[1, n], kgain)
        gk = gk + part
        send[2, n] = grad
    send_step(jnp.int32(STEPS - 1))
    sums[0] = jnp.concatenate([gq_ref[...], gk], axis=0)
    for n in range(MEMBERS):
        send[3, n] = dv_ref[n * TOK : (n + 1) * TOK, :].astype(BF16)
    for e in range(len(kin)):
        exchange(e).start()
        if e == len(kin) - 1:
            for n in range(3 * e, MEMBERS):
                results(3, n)
            for n in range(MEMBERS - HELD):
                results(2, n)
        exchange(e).wait_recv()
        sums[e + 1] = sums[e] + others[e]
        if e < len(kin) - 1:
            for n in range(3 * e, 3 * e + 3):
                results(3, n)
    wholes[me] = sums[len(kin)]
    for n in range(MEMBERS - HELD, MEMBERS - HELD + 2):
        results(2, n)
    for n in range(1, MEMBERS):
        publish(n).start()
    for n in range(MEMBERS - HELD + 2, MEMBERS):
        results(2, n)
    for n in range(1, MEMBERS):
        publish(n).wait_recv()
    for h in range(HEADS):
        gains_ref[:, h * HEAD : (h + 1) * HEAD] = wholes[h]

    for n in range(1, MEMBERS):
        publish(n).wait_send()
        for a in range(5):
            arrival(a, n, targets[n]).wait_send()
    for e in range(len(kin)):
        exchange(e).wait_send()
    for i in range(4):
        stays(i).wait()
    for n in range(1, MEMBERS):
        yy, zz = targets[n]
        for i in range(4):
            back(i, n, (yy, zz), yy * 8 + zz).wait()


def hand_over(*refs):
    sems = refs[-1]
    copies = [pltpu.make_async_copy(refs[i], refs[5 + i], sems.at[i]) for i in range(5)]
    for copy in copies:
        copy.start()
    for copy in copies:
        copy.wait()


def body(query_rows, key_rows, value_rows, cotangent, query_gain, key_gain, positions, span_start, span_length):
    rows = query_rows.shape[0]
    vmem = pl.BlockSpec(memory_space=pltpu.VMEM)
    hbm = pl.BlockSpec(memory_space=pltpu.HBM)
    free = pl.BlockSpec(memory_space=pl.ANY)
    row_array = jax.ShapeDtypeStruct((rows, HEADS * HEAD), BF16)
    dma = pltpu.SemaphoreType.DMA
    results = row_array, row_array, row_array, row_array, jax.ShapeDtypeStruct((2, HEADS * HEAD), F32)
    landed = pl.pallas_call(
        fused_kernel,
        out_shape=results,
        in_specs=[hbm] * 9,
        out_specs=(free,) * 4 + (vmem,),
        scratch_shapes=[
            pltpu.VMEM((4, MEMBERS, TOK, HEAD), BF16),
            pltpu.VMEM((MEMBERS, 1, TOK), jnp.int32),
            pltpu.VMEM((4, MEMBERS, TOK, HEAD), BF16),
            pltpu.VMEM((LEN, HEAD), BF16),
            pltpu.VMEM((HEAD, LEN), BF16),
            pltpu.VMEM((HEAD, LEN), BF16),
            pltpu.VMEM((LEN, 128), F32),
            pltpu.VMEM((STEPS, 1, QB), F32),
            pltpu.VMEM((LEN, QB), F32),
            pltpu.VMEM((LEN, QB), BF16),
            pltpu.VMEM((LEN, HEAD), F32),
            pltpu.VMEM((LEN, HEAD), F32),
            pltpu.VMEM((1, HEAD), F32),
            pltpu.VMEM((5, 2, HEAD), F32),
            pltpu.VMEM((4, 2, HEAD), F32),
            pltpu.VMEM((MEMBERS, 2, HEAD), F32),
            pltpu.SMEM((SEQS, SPANS), jnp.int32),
            pltpu.SMEM((SEQS, SPANS), jnp.int32),
            pltpu.VMEM((1, HEAD), F32),
            pltpu.VMEM((1, HEAD), F32),
            dma((4,)),
            dma((5, MEMBERS)),
            dma((5, MEMBERS)),
            dma((4, MEMBERS)),
            dma((4, MEMBERS)),
            dma((4,)),
            dma((4,)),
            dma((MEMBERS,)),
            dma((MEMBERS,)),
            pltpu.SemaphoreType.REGULAR((4,)),
        ],
        compiler_params=pltpu.CompilerParams(
            collective_id=0, has_side_effects=True, vmem_limit_bytes=GRANT
        ),
    )(
        *(
            pltpu.with_memory_space_constraint(t, pltpu.HBM)
            for t in (
                span_start, span_length, query_rows, key_rows, value_rows, cotangent,
                positions.reshape(1, TOK), query_gain.reshape(HEADS, HEAD), key_gain.reshape(HEADS, HEAD),
            )
        )
    )
    return pl.pallas_call(
        hand_over,
        out_shape=results,
        in_specs=[free] * 5,
        out_specs=(hbm,) * 5,
        scratch_shapes=[dma((5,))],
        compiler_params=pltpu.CompilerParams(vmem_limit_bytes=1 << 20),
    )(*landed)


def solution(mesh):
    split = Mesh(mesh.devices.reshape(2, 4, 2, 8, 2), DP_CTX)
    rows = P(DP_CTX, None)
    return jax.shard_map(
        body,
        mesh=split,
        in_specs=(rows, rows, rows, rows, P(), P(), P(DP_CTX), P(DP, None), P(DP, None)),
        out_specs=(rows, rows, rows, rows, P()),
        check_vma=False,
    )
```
